512 devices in a mesh: lat: 32 (over y, x), lon: 16 (over z, core).
Axes of the slice: x: 4, y: 8, z: 8, core: 2. Of those that a mesh axis runs over, the one named last changes fastest.
Arguments:
- pressure: float32 [1024, 512, 128], P('lat', 'lon'), may hold values from 0.2 to 1.8
- earlier: float32 [1024, 512, 128], P('lat', 'lon'), may hold values from 0.2 to 1.8
- speed_square: float32 [1024, 512, 128], P('lat', 'lon'), may hold values from 0.05 to 0.4
Outputs:
- potential: float32 [1024, 512, 128], P('lat', 'lon')
- pressure_end: float32 [1024, 512, 128], P('lat', 'lon')
The draws below stay inside these ranges and needn't reach their ends.
All inputs are finite; a program needn't handle non-finite values.
Results may differ from the reference program's by a relative error of at most 0.00002.
Values sent between devices are 32-bit elements; how exact they have to be, the bound alone decides.
No kernel may reach another device: no remote copies, remote signals or barrier semaphores. Data moves between devices by JAX's collectives and lax.ppermute only.
A program may use at most 64 MiB of HBM per device.

```python
import jax
import jax.numpy as jnp
from jax import lax

GRID_Y = 1024
GRID_X = 512
MEMBERS = 128
STEPS = 4


def block_scale(stream_key, shape, cuts, smallest, largest):
    factor_of = 1.0
    for dim, blocks in cuts:
        draws = jax.random.uniform(jax.random.fold_in(jax.random.fold_in(stream_key, 6), dim), (blocks,), jnp.float32, smallest / len(cuts), largest / len(cuts))
        factor_of = factor_of * jnp.repeat(jnp.exp(draws), shape[dim] // blocks).reshape((-1,) + (1,) * (len(shape) - 1 - dim))
    return factor_of


def setup_inputs(seed: int = 0) -> dict:
    seeds = jax.random.split(jax.random.key(seed), 4)
    pressure = jnp.clip(0.2 + 1.5999999 * jax.random.uniform(seeds[0], (GRID_Y, GRID_X, MEMBERS), jnp.float32) ** block_scale(seeds[0], (GRID_Y, GRID_X, MEMBERS), ((0, 32), (1, 16)), -0.2, 0.2), 0.2, 1.8)
    earlier = jnp.clip(0.2 + 1.5999999 * jax.random.uniform(seeds[1], (GRID_Y, GRID_X, MEMBERS), jnp.float32) ** block_scale(seeds[1], (GRID_Y, GRID_X, MEMBERS), ((0, 32), (1, 16)), -0.2, 0.2), 0.2, 1.8)
    speed_square = jnp.clip(0.05 + 0.35 * jax.random.uniform(seeds[2], (GRID_Y, GRID_X, MEMBERS), jnp.float32) ** block_scale(seeds[2], (GRID_Y, GRID_X, MEMBERS), ((0, 32), (1, 16)), -0.2, 0.2), 0.05, 0.4)
    return {"pressure": pressure, "earlier": earlier, "speed_square": speed_square}


def strip_edges(values, dims):
    for dim in dims:
        values = lax.slice_in_dim(values, 1, values.shape[dim] - 1, axis=dim)
    return values


def neighbour(values, dim, start, dims):
    others = [other for other in dims if other != dim]
    values = strip_edges(values, others)
    return lax.slice_in_dim(values, start, start + values.shape[dim] - 2, axis=dim)


def one_step(padded, before, speed_square):
    middle = strip_edges(padded, (0, 1))
    lower = [neighbour(padded, dim, 0, (0, 1)) for dim in (0, 1)]
    upper = [neighbour(padded, dim, 2, (0, 1)) for dim in (0, 1)]
    spread = lower[0] + upper[0] + lower[1] + upper[1] - 4.0 * middle
    return 2.0 * middle - before + speed_square * spread


def reference(pressure, earlier, speed_square):
    for step in range(STEPS):
        later = one_step(jnp.pad(pressure, ((1, 1), (1, 1), (0, 0)), mode="constant"), earlier, speed_square)
        earlier, pressure = pressure, later
    potential = jnp.cumsum(pressure, axis=0) / GRID_Y
    return potential, pressure
```

```python
import jax
import jax.numpy as jnp
from jax import lax
from jax.sharding import Mesh, PartitionSpec as P

STEPS = 4
LAT = ("y", "x")
LON = ("z", "core")


def padded_2(block, sides, width):
    for axis, dim in sides:
        count = lax.axis_size(axis)
        forward = [(i, i + 1) for i in range(count - 1)]
        backward = [(target, source) for source, target in forward]
        low = lax.ppermute(
            lax.slice_in_dim(block, block.shape[dim] - width, None, axis=dim), axis, forward
        )
        high = lax.ppermute(lax.slice_in_dim(block, 0, width, axis=dim), axis, backward)
        block = jnp.concatenate([low, block, high], axis=dim)
    return block


def all_of(array, axis):
    devices = lax.axis_size(axis)
    copies = jnp.broadcast_to(array, (devices, *array.shape[1:]))
    return lax.all_to_all(copies, axis, 0, 0, tiled=True)


def before(pieces, axis):
    passed = jnp.arange(pieces.shape[0]) < lax.axis_index(axis)
    return jnp.sum(jnp.where(passed.reshape(-1, 1, 1), pieces, 0.0), axis=0, keepdims=True)


def carried_in(total):
    row = all_of(total, "x")
    rows = all_of(jnp.sum(row, axis=0, keepdims=True), "y")
    return before(row, "x") + before(rows, "y")


def strip_edges(values, dims):
    for dim in dims:
        values = lax.slice_in_dim(values, 1, values.shape[dim] - 1, axis=dim)
    return values


def neighbour(values, dim, start, dims):
    others = [other for other in dims if other != dim]
    values = strip_edges(values, others)
    return lax.slice_in_dim(values, start, start + values.shape[dim] - 2, axis=dim)


def one_step(padded, before, speed_square):
    middle = strip_edges(padded, (0, 1))
    lower = [neighbour(padded, dim, 0, (0, 1)) for dim in (0, 1)]
    upper = [neighbour(padded, dim, 2, (0, 1)) for dim in (0, 1)]
    spread = lower[0] + upper[0] + lower[1] + upper[1] - 4.0 * middle
    return 2.0 * middle - before + speed_square * spread


def on_device(pressure, earlier, speed_square):
    padded = padded_2(pressure, ((LAT, 0), (LON, 1)), STEPS)
    wide_parts = padded_2(
        jnp.concatenate([earlier, speed_square], axis=2), ((LAT, 0), (LON, 1)), STEPS - 1
    )
    wide_earlier, wide_speed_square = jnp.split(wide_parts, 2, axis=2)
    for step in range(STEPS):
        later = one_step(padded, wide_earlier, wide_speed_square)
        values = later
        margin = STEPS - 1 - step
        place = lax.axis_index(LAT) * pressure.shape[0] - margin + jnp.arange(values.shape[0])
        keep_cells = (place >= 0) & (place < pressure.shape[0] * lax.axis_size(LAT))
        values = jnp.where(keep_cells.reshape((-1,) + (1,) * 2), values, 0.0)
        place = lax.axis_index(LON) * pressure.shape[1] - margin + jnp.arange(values.shape[1])
        keep_cells = (place >= 0) & (place < pressure.shape[1] * lax.axis_size(LON))
        values = jnp.where(keep_cells.reshape((-1,) + (1,) * 1), values, 0.0)
        later = values
        before = strip_edges(padded, (0, 1))
        if step < STEPS - 1:
            wide_earlier = strip_edges(before, (0, 1))
            wide_speed_square = strip_edges(wide_speed_square, (0, 1))
        padded = later
    pressure = padded
    here = jnp.cumsum(pressure, axis=0)
    total = lax.slice_in_dim(here, here.shape[0] - 1, here.shape[0], axis=0)

    below = carried_in(total)
    potential = (here + below) / (pressure.shape[0] * lax.axis_size(LAT))
    return (potential, pressure)


def solution(mesh):
    fine = Mesh(mesh.devices.reshape(8, 4, 8, 2), ("y", "x", "z", "core"))
    spec = P(LAT, LON, None)
    return jax.shard_map(
        on_device, mesh=fine, in_specs=(spec,) * 3, out_specs=(spec,) * 2, check_vma=False
    )
```

```python
import jax
import jax.numpy as jnp
from jax import lax
from jax.experimental import pallas as pl
from jax.experimental.pallas import tpu as pltpu
from jax.sharding import Mesh, PartitionSpec as P

STEPS = 4
ROWS, COLS, MEMBERS = 32, 32, 128
PITCH = 48
LEFT = 8
HALO = STEPS
TALL = ROWS + 2 * HALO
WIDE = COLS + 2 * HALO
DEPTHS = (HALO, HALO - 1, HALO - 1)
DEEP = sum(DEPTHS)
LAT = ("y", "x")
LON = ("z", "core")

HBM = pl.BlockSpec(memory_space=pltpu.HBM)
VMEM = pl.BlockSpec(memory_space=pltpu.VMEM)
PADDED = pltpu.VMEM((TALL, PITCH, MEMBERS), jnp.float32)


def in_vmem(*shape):
    return pltpu.VMEM((*shape, MEMBERS), jnp.float32)


def flat(ref):
    return ref.reshape(ref.shape[0] * ref.shape[1], MEMBERS)


def call(kernel, outs, name, args, specs, out_specs, scratch=(), aliases=None):
    return pl.pallas_call(
        kernel,
        out_shape=outs,
        in_specs=specs,
        out_specs=out_specs,
        scratch_shapes=scratch,
        input_output_aliases=aliases or {},
        name=name,
        compiler_params=pltpu.CompilerParams(vmem_limit_bytes=16 * 2**20),
    )(*args)


def cell(row, col):
    return (row + HALO) * PITCH + LEFT + col


def columns_to_message(padded, message, at_start):
    slot = 0
    for ref, depth in zip(padded, DEPTHS):
        first = jnp.where(at_start, 0, COLS - depth)
        for k in range(depth):
            message[pl.ds(slot * ROWS, ROWS), :] = flat(ref)[pl.ds(cell(0, first + k), ROWS, stride=PITCH), :]
            slot += 1


def message_to_columns(padded, message, at_start):
    slot = 0
    for ref, depth in zip(padded, DEPTHS):
        first = jnp.where(at_start, -depth, COLS)
        for k in range(depth):
            flat(ref)[pl.ds(cell(0, first + k), ROWS, stride=PITCH), :] = message[pl.ds(slot * ROWS, ROWS), :]
            slot += 1


def rows_to_message(padded, message, at_start):
    slot = 0
    for ref, depth in zip(padded, DEPTHS):
        first = jnp.where(at_start, 0, ROWS - depth)
        for k in range(depth):
            message[slot] = ref[first + k + HALO, LEFT - HALO : LEFT - HALO + WIDE, :]
            slot += 1


def message_to_rows(padded, message, at_start):
    slot = 0
    for ref, depth in zip(padded, DEPTHS):
        first = jnp.where(at_start, -depth, ROWS)
        for k in range(depth):
            ref[first + k + HALO, LEFT - HALO : LEFT - HALO + WIDE, :] = message[slot]
            slot += 1


def load_kernel(pressure, earlier, speed, *refs):
    padded, (outer, inner), sems = refs[:3], refs[3:5], refs[5]
    copies = [
        pltpu.make_async_copy(
            source, target.at[pl.ds(HALO, ROWS), pl.ds(LEFT, COLS), :], sems.at[i]
        )
        for i, (source, target) in enumerate(zip((pressure, earlier, speed), padded))
    ]
    for copy in copies:
        copy.start()
    for copy in copies:
        copy.wait()
    first_core = lax.axis_index("core") == 0
    columns_to_message(padded, outer, first_core)
    columns_to_message(padded, inner, jnp.logical_not(first_core))


def columns_kernel(_p, _e, _s, outer, inner, *refs):
    padded, (even, odd) = refs[:3], refs[3:5]
    first_core = lax.axis_index("core") == 0
    message_to_columns(padded, outer, first_core)
    message_to_columns(padded, inner, jnp.logical_not(first_core))
    odd_x = lax.axis_index("x") % 2 == 1
    rows_to_message(padded, even, odd_x)
    rows_to_message(padded, odd, jnp.logical_not(odd_x))


def later_row(source, before, speed, row, first, width):
    cells = slice(first, first + width)
    middle = source[row, cells, :]
    spread = source[row - 1, cells, :] + source[row + 1, cells, :]
    spread += source[row, first - 1 : first - 1 + width, :]
    spread += source[row, first + 1 : first + 1 + width, :]
    spread -= 4.0 * middle
    return 2.0 * middle - before[row, cells, :] + speed[row, cells, :] * spread


def steps_kernel(_p, _e, _s, even, odd, *refs):
    padded, (end, sums, copies) = refs[:3], refs[3:6]
    odd_x = lax.axis_index("x") % 2 == 1
    message_to_rows(padded, even, odd_x)
    message_to_rows(padded, odd, jnp.logical_not(odd_x))
    now, before, speed = padded
    for step in range(STEPS - 1):
        margin = STEPS - 1 - step

        def pair(i, _, now=now, before=before, margin=margin):
            for k in range(2):
                row = HALO - margin + 2 * i + k
                before[row, LEFT - HALO : LEFT - HALO + WIDE, :] = later_row(
                    now, before, speed, row, LEFT - HALO, WIDE
                )
            return 0

        lax.fori_loop(0, (ROWS + 2 * margin) // 2, pair, 0)
        now, before = before, now

    def last(i, total):
        for k in range(2):
            row = 2 * i + k
            value = later_row(now, before, speed, row + HALO, LEFT, COLS)
            end[row] = value
            total = total + value
            sums[row] = total * (1.0 / 1024)
        return total

    total = lax.fori_loop(0, ROWS // 2, last, jnp.zeros((COLS, MEMBERS), jnp.float32))
    for k in range(copies.shape[0]):
        copies[k] = total


def middle_kernel(row, copies, before):
    here = lax.axis_index("x")
    total = jnp.zeros((COLS, MEMBERS), jnp.float32)
    for k in range(row.shape[0]):
        before[...] = jnp.where(k == here, total, before[...])
        total = total + row[k]
    for k in range(copies.shape[0]):
        copies[k] = total


def final_kernel(rows, before, sums, end, potential_out, end_out, potential, sems):
    end_copy = pltpu.make_async_copy(end, end_out, sems.at[0])
    end_copy.start()
    here = lax.axis_index("y")
    total = before[...]
    for k in range(rows.shape[0]):
        total = total + jnp.where(k < here, rows[k], 0.0)
    total = total * (1.0 / 1024)

    def add(i, _):
        for k in range(4):
            potential[4 * i + k] = sums[4 * i + k] + total
        return 0

    lax.fori_loop(0, ROWS // 4, add, 0)
    copy = pltpu.make_async_copy(potential, potential_out, sems.at[1])
    copy.start()
    copy.wait()
    end_copy.wait()


def on_device(pressure, earlier, speed_square):
    *padded, outer, inner = call(
        load_kernel,
        [PADDED] * 3 + [in_vmem(DEEP * ROWS)] * 2,
        "load",
        (pressure, earlier, speed_square),
        [HBM] * 3,
        [VMEM] * 5,
        [pltpu.SemaphoreType.DMA((3,))],
    )
    chips, ys, xs = (lax.axis_size(name) for name in ("z", "y", "x"))
    swap = lambda pairs: pairs + [(b, a) for a, b in pairs]
    outer = lax.ppermute(outer, LON, swap([(2 * z + 1, 2 * z + 2) for z in range(chips - 1)]))
    inner = lax.ppermute(inner, LON, swap([(2 * z, 2 * z + 1) for z in range(chips)]))
    same = {0: 0, 1: 1, 2: 2}
    *padded, even, odd = call(
        columns_kernel,
        [PADDED] * 3 + [in_vmem(DEEP, WIDE)] * 2,
        "columns",
        (*padded, outer, inner),
        [VMEM] * 5,
        [VMEM] * 5,
        aliases=same,
    )
    blocks = ys * xs
    even = lax.ppermute(even, LAT, swap([(i, i + 1) for i in range(0, blocks, 2)]))
    odd = lax.ppermute(odd, LAT, swap([(i, i + 1) for i in range(1, blocks - 1, 2)]))
    *_, end, sums, copies = call(
        steps_kernel,
        [PADDED] * 3 + [in_vmem(ROWS, COLS)] * 2 + [in_vmem(xs, COLS)],
        "steps",
        (*padded, even, odd),
        [VMEM] * 5,
        [VMEM] * 6,
        aliases=same,
    )
    row = lax.all_to_all(copies, "x", 0, 0, tiled=True)
    copies, before = call(
        middle_kernel,
        [in_vmem(ys, COLS), in_vmem(COLS)],
        "middle",
        (row,),
        [VMEM],
        [VMEM] * 2,
    )
    rows = lax.all_to_all(copies, "y", 0, 0, tiled=True)
    return call(
        final_kernel,
        [jax.ShapeDtypeStruct((ROWS, COLS, MEMBERS), jnp.float32)] * 2,
        "final",
        (rows, before, sums, end),
        [VMEM] * 4,
        [HBM] * 2,
        [pltpu.VMEM((ROWS, COLS, MEMBERS), jnp.float32), pltpu.SemaphoreType.DMA((2,))],
    )


def solution(mesh):
    fine = Mesh(mesh.devices.reshape(8, 4, 8, 2), ("y", "x", "z", "core"))
    spec = P(LAT, LON, None)
    return jax.shard_map(
        on_device, mesh=fine, in_specs=(spec,) * 3, out_specs=(spec,) * 2, check_vma=False
    )
```

```python
import jax
import jax.numpy as jnp
from jax import lax
from jax.experimental import pallas as pl
from jax.experimental.pallas import tpu as pltpu
from jax.sharding import Mesh, PartitionSpec as P

STEPS = 4
ROWS, COLS, MEMBERS = 32, 32, 128
PITCH = 48
LEFT = 8
HALO = STEPS
TALL = ROWS + 2 * HALO
WIDE = COLS + 2 * HALO
DEPTHS = (HALO, HALO - 1, HALO - 1)
DEEP = sum(DEPTHS)
PIECES = 4
LAT = ("y", "x")
LON = ("z", "core")

HBM = pl.BlockSpec(memory_space=pltpu.HBM)
VMEM = pl.BlockSpec(memory_space=pltpu.VMEM)
PADDED = pltpu.VMEM((TALL, PITCH, MEMBERS), jnp.float32)


def in_vmem(*shape):
    return pltpu.VMEM((*shape, MEMBERS), jnp.float32)


def flat(ref):
    return ref.reshape(ref.shape[0] * ref.shape[1], MEMBERS)


def call(kernel, outs, name, args, specs, out_specs, scratch=(), aliases=None):
    return pl.pallas_call(
        kernel,
        out_shape=outs,
        in_specs=specs,
        out_specs=out_specs,
        scratch_shapes=scratch,
        input_output_aliases=aliases or {},
        name=name,
        compiler_params=pltpu.CompilerParams(vmem_limit_bytes=16 * 2**20),
    )(*args)


def cell(row, col):
    return (row + HALO) * PITCH + LEFT + col


def columns_to_message(padded, message, at_start):
    slot = 0
    for ref, depth in zip(padded, DEPTHS):
        first = jnp.where(at_start, 0, COLS - depth)
        for k in range(depth):
            message[pl.ds(slot * ROWS, ROWS), :] = flat(ref)[pl.ds(cell(0, first + k), ROWS, stride=PITCH), :]
            slot += 1


def message_to_columns(padded, message, at_start):
    slot = 0
    for ref, depth in zip(padded, DEPTHS):
        first = jnp.where(at_start, -depth, COLS)
        for k in range(depth):
            flat(ref)[pl.ds(cell(0, first + k), ROWS, stride=PITCH), :] = message[pl.ds(slot * ROWS, ROWS), :]
            slot += 1


def rows_to_message(padded, message, at_start):
    slot = 0
    for ref, depth in zip(padded, DEPTHS):
        first = jnp.where(at_start, 0, ROWS - depth)
        for k in range(depth):
            message[slot] = ref[first + k + HALO, LEFT - HALO : LEFT - HALO + WIDE, :]
            slot += 1


def message_to_rows(padded, message, at_start):
    slot = 0
    for ref, depth in zip(padded, DEPTHS):
        first = jnp.where(at_start, -depth, ROWS)
        for k in range(depth):
            ref[first + k + HALO, LEFT - HALO : LEFT - HALO + WIDE, :] = message[slot]
            slot += 1


def load_kernel(pressure, earlier, speed, *refs):
    padded, (outer, inner), sems = refs[:3], refs[3:5], refs[5]
    piece = ROWS // PIECES
    copies = [
        pltpu.make_async_copy(
            source.at[pl.ds(k * piece, piece)],
            target.at[pl.ds(HALO + k * piece, piece), pl.ds(LEFT, COLS), :],
            sems.at[i, k],
        )
        for i, (source, target) in enumerate(zip((pressure, earlier, speed), padded))
        for k in range(PIECES)
    ]
    for copy in copies:
        copy.start()
    for copy in copies:
        copy.wait()
    first_core = lax.axis_index("core") == 0
    columns_to_message(padded, outer, first_core)
    columns_to_message(padded, inner, jnp.logical_not(first_core))


def columns_kernel(_p, _e, _s, outer, inner, *refs):
    padded, (even, odd) = refs[:3], refs[3:5]
    first_core = lax.axis_index("core") == 0
    message_to_columns(padded, outer, first_core)
    message_to_columns(padded, inner, jnp.logical_not(first_core))
    odd_x = lax.axis_index("x") % 2 == 1
    rows_to_message(padded, even, odd_x)
    rows_to_message(padded, odd, jnp.logical_not(odd_x))


def later_row(source, before, speed, row, first, width):
    cells = slice(first, first + width)
    middle = source[row, cells, :]
    spread = source[row - 1, cells, :] + source[row + 1, cells, :]
    spread += source[row, first - 1 : first - 1 + width, :]
    spread += source[row, first + 1 : first + 1 + width, :]
    spread -= 4.0 * middle
    return 2.0 * middle - before[row, cells, :] + speed[row, cells, :] * spread


def steps_kernel(_p, _e, _s, odd, even, *refs):
    padded, (end, sums, copies) = refs[:3], refs[3:6]
    odd_x = lax.axis_index("x") % 2 == 1
    message_to_rows(padded, even, odd_x)
    message_to_rows(padded, odd, jnp.logical_not(odd_x))
    now, before, speed = padded
    for step in range(STEPS - 1):
        margin = STEPS - 1 - step

        def pair(i, _, now=now, before=before, margin=margin):
            for k in range(2):
                row = HALO - margin + 2 * i + k
                before[row, LEFT - HALO : LEFT - HALO + WIDE, :] = later_row(
                    now, before, speed, row, LEFT - HALO, WIDE
                )
            return 0

        lax.fori_loop(0, (ROWS + 2 * margin) // 2, pair, 0)
        now, before = before, now

    def last(i, total):
        for k in range(2):
            row = 2 * i + k
            value = later_row(now, before, speed, row + HALO, LEFT, COLS)
            end[row] = value
            total = total + value
            sums[row] = total * (1.0 / 1024)
        return total

    total = lax.fori_loop(0, ROWS // 2, last, jnp.zeros((COLS, MEMBERS), jnp.float32))
    for k in range(copies.shape[0]):
        copies[k] = total


def middle_kernel(row, copies, before):
    here = lax.axis_index("x")
    total = jnp.zeros((COLS, MEMBERS), jnp.float32)
    for k in range(row.shape[0]):
        before[...] = jnp.where(k == here, total, before[...])
        total = total + row[k]
    for k in range(copies.shape[0]):
        copies[k] = total


def final_kernel(rows, before, sums, end, potential_out, end_out, potential, sems):
    end_copy = pltpu.make_async_copy(end, end_out, sems.at[0])
    end_copy.start()
    here = lax.axis_index("y")
    total = before[...]
    for k in range(rows.shape[0]):
        total = total + jnp.where(k < here, rows[k], 0.0)
    total = total * (1.0 / 1024)

    def add(i, _):
        for k in range(4):
            potential[4 * i + k] = sums[4 * i + k] + total
        return 0

    lax.fori_loop(0, ROWS // 4, add, 0)
    copy = pltpu.make_async_copy(potential, potential_out, sems.at[1])
    copy.start()
    copy.wait()
    end_copy.wait()


def on_device(pressure, earlier, speed_square):
    *padded, outer, inner = call(
        load_kernel,
        [PADDED] * 3 + [in_vmem(DEEP * ROWS)] * 2,
        "load",
        [pltpu.with_memory_space_constraint(a, pltpu.HBM) for a in (pressure, earlier, speed_square)],
        [HBM] * 3,
        [VMEM] * 5,
        [pltpu.SemaphoreType.DMA((3, PIECES))],
    )
    chips, ys, xs = (lax.axis_size(name) for name in ("z", "y", "x"))
    swap = lambda pairs: pairs + [(b, a) for a, b in pairs]
    outer = lax.ppermute(outer, LON, swap([(2 * z + 1, 2 * z + 2) for z in range(chips - 1)]))
    inner = lax.ppermute(inner, LON, swap([(2 * z, 2 * z + 1) for z in range(chips)]))
    same = {0: 0, 1: 1, 2: 2}
    *padded, even, odd = call(
        columns_kernel,
        [PADDED] * 3 + [in_vmem(DEEP, WIDE)] * 2,
        "columns",
        (*padded, outer, inner),
        [VMEM] * 5,
        [VMEM] * 5,
        aliases=same,
    )
    blocks = ys * xs
    odd = lax.ppermute(odd, LAT, swap([(i, i + 1) for i in range(1, blocks - 1, 2)]))
    even = lax.ppermute(even, LAT, swap([(i, i + 1) for i in range(0, blocks, 2)]))
    *_, end, sums, copies = call(
        steps_kernel,
        [PADDED] * 3 + [in_vmem(ROWS, COLS)] * 2 + [in_vmem(xs, COLS)],
        "steps",
        (*padded, odd, even),
        [VMEM] * 5,
        [VMEM] * 6,
        aliases=same,
    )
    row = lax.all_to_all(copies, "x", 0, 0, tiled=True)
    copies, before = call(
        middle_kernel,
        [in_vmem(ys, COLS), in_vmem(COLS)],
        "middle",
        (row,),
        [VMEM],
        [VMEM] * 2,
    )
    rows = lax.all_to_all(copies, "y", 0, 0, tiled=True)
    return call(
        final_kernel,
        [jax.ShapeDtypeStruct((ROWS, COLS, MEMBERS), jnp.float32)] * 2,
        "final",
        (rows, before, sums, end),
        [VMEM] * 4,
        [HBM] * 2,
        [pltpu.VMEM((ROWS, COLS, MEMBERS), jnp.float32), pltpu.SemaphoreType.DMA((2,))],
    )


def solution(mesh):
    fine = Mesh(mesh.devices.reshape(8, 4, 8, 2), ("y", "x", "z", "core"))
    spec = P(LAT, LON, None)
    return jax.shard_map(
        on_device, mesh=fine, in_specs=(spec,) * 3, out_specs=(spec,) * 2, check_vma=False
    )
```

```python
import jax
import jax.numpy as jnp
from jax import lax
from jax.experimental import pallas as pl
from jax.experimental.pallas import tpu as pltpu
from jax.sharding import Mesh, PartitionSpec as P

STEPS = 4
ROWS, COLS, MEMBERS = 32, 32, 128
PITCH = 56
LEFT = 8
HALO = STEPS
TALL = ROWS + 2 * HALO
WIDE = COLS + 2 * HALO
DEPTHS = (HALO, HALO - 1, HALO - 1)
DEEP = sum(DEPTHS)
PIECES = 4
FINAL_PIECES = 4
INSIDE = ROWS - 2 * STEPS
SCALE = 1.0 / 1024
LAT = ("y", "x")
LON = ("z", "core")

HBM = pl.BlockSpec(memory_space=pltpu.HBM)
VMEM = pl.BlockSpec(memory_space=pltpu.VMEM)
WHOLE = pltpu.HBM((ROWS, COLS, MEMBERS), jnp.float32)
PADDED = pltpu.VMEM((TALL, PITCH, MEMBERS), jnp.float32)


def in_vmem(*shape):
    return pltpu.VMEM((*shape, MEMBERS), jnp.float32)


def flat(ref):
    return ref.reshape(ref.shape[0] * ref.shape[1], MEMBERS)


def call(kernel, outs, name, args, specs, out_specs, scratch=(), aliases=None, flops=10**5):
    return pl.pallas_call(
        kernel,
        out_shape=outs,
        in_specs=specs,
        out_specs=out_specs,
        scratch_shapes=scratch,
        input_output_aliases=aliases or {},
        name=name,
        cost_estimate=pl.CostEstimate(flops=flops, bytes_accessed=0, transcendentals=0),
        compiler_params=pltpu.CompilerParams(vmem_limit_bytes=16 * 2**20),
    )(*args)


def cell(row, col):
    return (row + HALO) * PITCH + LEFT + col


def columns_to_message(padded, message, at_start):
    slot = 0
    for ref, depth in zip(padded, DEPTHS):
        first = jnp.where(at_start, 0, COLS - depth)
        for k in range(depth):
            message[pl.ds(slot * ROWS, ROWS), :] = flat(ref)[pl.ds(cell(0, first + k), ROWS, stride=PITCH), :]
            slot += 1


def message_to_columns(padded, message, at_start):
    slot = 0
    for ref, depth in zip(padded, DEPTHS):
        first = jnp.where(at_start, -depth, COLS)
        for k in range(depth):
            flat(ref)[pl.ds(cell(0, first + k), ROWS, stride=PITCH), :] = message[pl.ds(slot * ROWS, ROWS), :]
            slot += 1


def rows_to_message(padded, message, at_start):
    now, before, speed = padded
    first, second, third = (HALO + jnp.where(at_start, k, ROWS - 1 - k) for k in range(3))
    cells = slice(LEFT - HALO, LEFT - HALO + WIDE)
    beyond = speed[second, cells, :] * later_row(now, before, speed, third, LEFT - HALO, WIDE)
    message[0] = now[first, cells, :]
    message[1] = now[second, cells, :] - beyond
    message[2] = before[first, cells, :] - speed[first, cells, :] * beyond
    message[3] = later_row(now, before, speed, second, LEFT - HALO, WIDE)
    message[4] = speed[first, cells, :]
    message[5] = speed[second, cells, :]


def message_to_rows(padded, message, at_start):
    for k in range(2):
        row = HALO + jnp.where(at_start, -1 - k, ROWS + k)
        for slot, ref in enumerate(padded):
            ref[row, LEFT - HALO : LEFT - HALO + WIDE, :] = message[2 * slot + k]


def load_kernel(pressure, earlier, speed, *refs):
    padded, (outer, inner), sems = refs[:3], refs[3:5], refs[5]
    piece = ROWS // PIECES
    copies = [
        pltpu.make_async_copy(
            source.at[pl.ds(k * piece, piece)],
            target.at[pl.ds(HALO + k * piece, piece), pl.ds(LEFT, COLS), :],
            sems.at[i, k],
        )
        for i, (source, target) in enumerate(zip((pressure, earlier, speed), padded))
        for k in range(PIECES)
    ]
    for copy in copies:
        copy.start()
    for copy in copies:
        copy.wait()
    first_core = lax.axis_index("core") == 0
    columns_to_message(padded, outer, first_core)
    columns_to_message(padded, inner, jnp.logical_not(first_core))


def columns_kernel(_p, _e, _s, outer, inner, *refs):
    padded, (odd, even) = refs[:3], refs[3:5]
    first_core = lax.axis_index("core") == 0
    message_to_columns(padded, outer, first_core)
    message_to_columns(padded, inner, jnp.logical_not(first_core))
    odd_x = lax.axis_index("x") % 2 == 1
    rows_to_message(padded, odd, jnp.logical_not(odd_x))
    rows_to_message(padded, even, odd_x)
    for row in (HALO - 3, HALO + ROWS + 2):
        padded[1][row] = jnp.zeros((PITCH, MEMBERS), jnp.float32)


def later_row(source, before, speed, row, first, width):
    cells = slice(first, first + width)
    middle = source[row, cells, :]
    spread = source[row - 1, cells, :] + source[row + 1, cells, :]
    spread += source[row, first - 1 : first - 1 + width, :]
    spread += source[row, first + 1 : first + 1 + width, :]
    spread -= 4.0 * middle
    return 2.0 * middle - before[row, cells, :] + speed[row, cells, :] * spread


def set_later_row(source, before, speed, row):
    cells = slice(LEFT - HALO, LEFT - HALO + WIDE)
    before[row, cells, :] = later_row(source, before, speed, row, LEFT - HALO, WIDE)


def inner_kernel(_p, _e, _s, *refs):
    padded, (end_out, sums, total_out, end, sem) = refs[:3], refs[3:]
    now, before, speed = padded
    for step in range(1, STEPS):

        def pair(i, _, now=now, before=before, step=step):
            for k in range(2):
                set_later_row(now, before, speed, HALO + step + 2 * i + k)
            return 0

        lax.fori_loop(0, (ROWS - 2 * step) // 2, pair, 0)
        now, before = before, now

    def last(i, total):
        for k in range(2):
            row = 2 * i + k
            value = later_row(now, before, speed, row + HALO + STEPS, LEFT, COLS)
            end[row] = value
            total = total + value
            sums[row] = total * SCALE
        return total

    total_out[...] = lax.fori_loop(0, INSIDE // 2, last, jnp.zeros((COLS, MEMBERS), jnp.float32))
    copy = pltpu.make_async_copy(end, end_out.at[pl.ds(STEPS, INSIDE)], sem)
    copy.start()
    copy.wait()


def edges_kernel(_p, _e, _s, odd, even, inside, *refs):
    padded, (end, sums, offsets, copies) = refs[:3], refs[3:]
    odd_x = lax.axis_index("x") % 2 == 1
    message_to_rows(padded, odd, jnp.logical_not(odd_x))
    message_to_rows(padded, even, odd_x)
    now, before, speed = padded
    for first, count in ((-1, 2), (-2, 4), (-1, 4)):
        for k in range(count):
            set_later_row(now, before, speed, HALO + first + k)
            set_later_row(now, before, speed, HALO + ROWS - 1 - first - k)
        now, before = before, now
    total = jnp.zeros((COLS, MEMBERS), jnp.float32)
    for side in range(2):
        here = jnp.zeros((COLS, MEMBERS), jnp.float32)
        for k in range(STEPS):
            row = side * (ROWS - STEPS) + k
            value = later_row(now, before, speed, row + HALO, LEFT, COLS)
            end[side * STEPS + k] = value
            here = here + value
            sums[side * STEPS + k] = here * SCALE
        total = total + here
        if side == 0:
            offsets[0] = total * SCALE
            total = total + inside[...]
            offsets[1] = total * SCALE
    for k in range(copies.shape[0]):
        copies[k] = total


def middle_kernel(row, copies, before):
    here = lax.axis_index("x")
    total = jnp.zeros((COLS, MEMBERS), jnp.float32)
    for k in range(row.shape[0]):
        before[...] = jnp.where(k == here, total, before[...])
        total = total + row[k]
    for k in range(copies.shape[0]):
        copies[k] = total


def final_kernel(rows, before, inner_sums, edge_sums, offsets, edges, _end, potential_out, end_out, potential, sems):
    copies = [
        pltpu.make_async_copy(edges.at[pl.ds(0, STEPS)], end_out.at[pl.ds(0, STEPS)], sems.at[0]),
        pltpu.make_async_copy(
            edges.at[pl.ds(STEPS, STEPS)], end_out.at[pl.ds(ROWS - STEPS, STEPS)], sems.at[1]
        ),
    ]
    for copy in copies:
        copy.start()
    here = lax.axis_index("y")
    total = before[...]
    for k in range(rows.shape[0]):
        total = total + jnp.where(k < here, rows[k], 0.0)
    total = total * SCALE
    upper = total + offsets[1]
    for k in range(STEPS):
        potential[k] = edge_sums[k] + total
        potential[ROWS - STEPS + k] = edge_sums[STEPS + k] + upper
    inner = total + offsets[0]
    piece = ROWS // FINAL_PIECES
    for part in range(FINAL_PIECES):
        for row in range(part * piece, (part + 1) * piece):
            if STEPS <= row < ROWS - STEPS:
                potential[row] = inner_sums[row - STEPS] + inner
        place = pl.ds(part * piece, piece)
        copy = pltpu.make_async_copy(potential.at[place], potential_out.at[place], sems.at[2 + part])
        copy.start()
        copies.append(copy)
    for copy in copies:
        copy.wait()


def on_device(pressure, earlier, speed_square):
    *padded, outer, inner = call(
        load_kernel,
        [PADDED] * 3 + [in_vmem(DEEP * ROWS)] * 2,
        "load",
        [pltpu.with_memory_space_constraint(a, pltpu.HBM) for a in (pressure, earlier, speed_square)],
        [HBM] * 3,
        [VMEM] * 5,
        [pltpu.SemaphoreType.DMA((3, PIECES))],
    )
    chips, ys, xs = (lax.axis_size(name) for name in ("z", "y", "x"))
    swap = lambda pairs: pairs + [(b, a) for a, b in pairs]
    outer = lax.ppermute(outer, LON, swap([(2 * z + 1, 2 * z + 2) for z in range(chips - 1)]))
    inner = lax.ppermute(inner, LON, swap([(2 * z, 2 * z + 1) for z in range(chips)]))
    same = {0: 0, 1: 1, 2: 2}
    *padded, odd, even = call(
        columns_kernel,
        [PADDED] * 3 + [in_vmem(6, WIDE)] * 2,
        "columns",
        (*padded, outer, inner),
        [VMEM] * 5,
        [VMEM] * 5,
        aliases=same,
    )
    blocks = ys * xs
    odd = lax.ppermute(odd, LAT, swap([(i, i + 1) for i in range(1, blocks - 1, 2)]))
    even = lax.ppermute(even, LAT, swap([(i, i + 1) for i in range(0, blocks, 2)]))
    *padded, end, inner_sums, inside = call(
        inner_kernel,
        [PADDED] * 3 + [WHOLE, in_vmem(INSIDE, COLS), in_vmem(COLS)],
        "inner",
        padded,
        [VMEM] * 3,
        [VMEM] * 3 + [HBM] + [VMEM] * 2,
        [in_vmem(INSIDE, COLS), pltpu.SemaphoreType.DMA],
        aliases=same,
        flops=10**8,
    )
    *_, edges, edge_sums, offsets, copies = call(
        edges_kernel,
        [PADDED] * 3 + [in_vmem(2 * STEPS, COLS)] * 2 + [in_vmem(2, COLS), in_vmem(xs, COLS)],
        "edges",
        (*padded, odd, even, inside),
        [VMEM] * 6,
        [VMEM] * 7,
        aliases=same,
    )
    row = lax.all_to_all(copies, "x", 0, 0, tiled=True)
    copies, before = call(
        middle_kernel,
        [in_vmem(ys, COLS), in_vmem(COLS)],
        "middle",
        (row,),
        [VMEM],
        [VMEM] * 2,
    )
    rows = lax.all_to_all(copies, "y", 0, 0, tiled=True)
    return call(
        final_kernel,
        [WHOLE] * 2,
        "final",
        (rows, before, inner_sums, edge_sums, offsets, edges, end),
        [VMEM] * 6 + [HBM],
        [HBM] * 2,
        [in_vmem(ROWS, COLS), pltpu.SemaphoreType.DMA((2 + FINAL_PIECES,))],
        aliases={6: 1},
    )


def solution(mesh):
    fine = Mesh(mesh.devices.reshape(8, 4, 8, 2), ("y", "x", "z", "core"))
    spec = P(LAT, LON, None)
    return jax.shard_map(
        on_device, mesh=fine, in_specs=(spec,) * 3, out_specs=(spec,) * 2, check_vma=False
    )
```

```python
import jax
import jax.numpy as jnp
from jax import lax
from jax.experimental import pallas as pl
from jax.experimental.pallas import tpu as pltpu
from jax.sharding import Mesh, PartitionSpec as P

STEPS = 4
ROWS, COLS, MEMBERS = 32, 32, 128
PITCH = 56
LEFT = 8
HALO = STEPS
TALL = ROWS + 2 * HALO
WIDE = COLS + 2 * HALO
DEPTHS = (HALO, HALO - 1, HALO - 1)
DEEP = sum(DEPTHS)
PIECES = 4
FINAL_PIECES = 4
INSIDE = ROWS - 2 * STEPS
SCALE = 1.0 / 1024
LAT = ("y", "x")
LON = ("z", "core")

HBM = pl.BlockSpec(memory_space=pltpu.HBM)
VMEM = pl.BlockSpec(memory_space=pltpu.VMEM)
WHOLE = pltpu.HBM((ROWS, COLS, MEMBERS), jnp.float32)
PADDED = pltpu.VMEM((TALL, PITCH, MEMBERS), jnp.float32)


def in_vmem(*shape):
    return pltpu.VMEM((*shape, MEMBERS), jnp.float32)


def flat(ref):
    return ref.reshape(ref.shape[0] * ref.shape[1], MEMBERS)


def call(kernel, outs, name, args, specs, out_specs, scratch=(), aliases=None, flops=10**5):
    return pl.pallas_call(
        kernel,
        out_shape=outs,
        in_specs=specs,
        out_specs=out_specs,
        scratch_shapes=scratch,
        input_output_aliases=aliases or {},
        name=name,
        cost_estimate=pl.CostEstimate(flops=flops, bytes_accessed=0, transcendentals=0),
        compiler_params=pltpu.CompilerParams(vmem_limit_bytes=16 * 2**20),
    )(*args)


def cell(row, col):
    return (row + HALO) * PITCH + LEFT + col


def columns_to_message(padded, message, at_start):
    slot = 0
    for ref, depth in zip(padded, DEPTHS):
        first = jnp.where(at_start, 0, COLS - depth)
        for k in range(depth):
            message[pl.ds(slot * ROWS, ROWS), :] = flat(ref)[pl.ds(cell(0, first + k), ROWS, stride=PITCH), :]
            slot += 1


def message_to_columns(padded, message, at_start):
    slot = 0
    for ref, depth in zip(padded, DEPTHS):
        first = jnp.where(at_start, -depth, COLS)
        for k in range(depth):
            flat(ref)[pl.ds(cell(0, first + k), ROWS, stride=PITCH), :] = message[pl.ds(slot * ROWS, ROWS), :]
            slot += 1


def rows_to_message(padded, message, at_start):
    now, before, speed = padded
    first, second, third = (HALO + jnp.where(at_start, k, ROWS - 1 - k) for k in range(3))
    cells = slice(LEFT - HALO, LEFT - HALO + WIDE)
    beyond = speed[second, cells, :] * later_row(now, before, speed, third, LEFT - HALO, WIDE)
    message[0] = now[first, cells, :]
    message[1] = now[second, cells, :] - beyond
    message[2] = before[first, cells, :] - speed[first, cells, :] * beyond
    message[3] = later_row(now, before, speed, second, LEFT - HALO, WIDE)
    message[4] = speed[first, cells, :]
    message[5] = speed[second, cells, :]


def message_to_rows(padded, message, at_start):
    for k in range(2):
        row = HALO + jnp.where(at_start, -1 - k, ROWS + k)
        for slot, ref in enumerate(padded):
            ref[row, LEFT - HALO : LEFT - HALO + WIDE, :] = message[2 * slot + k]


def load_kernel(pressure, earlier, speed, *refs):
    padded, (outer, inner), sems = refs[:3], refs[3:5], refs[5]
    piece = ROWS // PIECES
    copies = [
        pltpu.make_async_copy(
            source.at[pl.ds(k * piece, piece)],
            target.at[pl.ds(HALO + k * piece, piece), pl.ds(LEFT, COLS), :],
            sems.at[i, k],
        )
        for i, (source, target) in enumerate(zip((pressure, earlier, speed), padded))
        for k in range(PIECES)
    ]
    for copy in copies:
        copy.start()
    for copy in copies:
        copy.wait()
    first_core = lax.axis_index("core") == 0
    columns_to_message(padded, outer, first_core)
    columns_to_message(padded, inner, jnp.logical_not(first_core))


def columns_kernel(_p, _e, _s, outer, inner, *refs):
    padded, (odd, even) = refs[:3], refs[3:5]
    first_core = lax.axis_index("core") == 0
    message_to_columns(padded, outer, first_core)
    message_to_columns(padded, inner, jnp.logical_not(first_core))
    odd_x = lax.axis_index("x") % 2 == 1
    rows_to_message(padded, odd, jnp.logical_not(odd_x))
    rows_to_message(padded, even, odd_x)
    for row in (HALO - 3, HALO + ROWS + 2):
        padded[1][row] = jnp.zeros((PITCH, MEMBERS), jnp.float32)


def later_row(source, before, speed, row, first, width):
    cells = slice(first, first + width)
    middle = source[row, cells, :]
    spread = source[row - 1, cells, :] + source[row + 1, cells, :]
    spread += source[row, first - 1 : first - 1 + width, :]
    spread += source[row, first + 1 : first + 1 + width, :]
    spread -= 4.0 * middle
    return 2.0 * middle - before[row, cells, :] + speed[row, cells, :] * spread


def set_later_row(source, before, speed, row):
    cells = slice(LEFT - HALO, LEFT - HALO + WIDE)
    before[row, cells, :] = later_row(source, before, speed, row, LEFT - HALO, WIDE)


def inner_kernel(_p, _e, _s, *refs):
    padded, (end_out, sums, total_out, end, sem) = refs[:3], refs[3:]
    now, before, speed = padded
    for step in range(1, STEPS):

        def pair(i, _, now=now, before=before, step=step):
            for k in range(2):
                set_later_row(now, before, speed, HALO + step + 2 * i + k)
            return 0

        lax.fori_loop(0, (ROWS - 2 * step) // 2, pair, 0)
        now, before = before, now

    def last(i, total):
        for k in range(2):
            row = 2 * i + k
            value = later_row(now, before, speed, row + HALO + STEPS, LEFT, COLS)
            end[row] = value
            total = total + value
            sums[row] = total * SCALE
        return total

    total_out[...] = lax.fori_loop(0, INSIDE // 2, last, jnp.zeros((COLS, MEMBERS), jnp.float32))
    copy = pltpu.make_async_copy(end, end_out.at[pl.ds(STEPS, INSIDE)], sem)
    copy.start()
    copy.wait()


def edges_kernel(_p, _e, _s, odd, even, inside, *refs):
    padded, (end, sums, offsets, copies) = refs[:3], refs[3:]
    odd_x = lax.axis_index("x") % 2 == 1
    message_to_rows(padded, odd, jnp.logical_not(odd_x))
    message_to_rows(padded, even, odd_x)
    now, before, speed = padded
    for first, count in ((-1, 2), (-2, 4), (-1, 4)):
        for k in range(count):
            set_later_row(now, before, speed, HALO + first + k)
            set_later_row(now, before, speed, HALO + ROWS - 1 - first - k)
        now, before = before, now
    total = jnp.zeros((COLS, MEMBERS), jnp.float32)
    for side in range(2):
        here = jnp.zeros((COLS, MEMBERS), jnp.float32)
        for k in range(STEPS):
            row = side * (ROWS - STEPS) + k
            value = later_row(now, before, speed, row + HALO, LEFT, COLS)
            end[side * STEPS + k] = value
            here = here + value
            sums[side * STEPS + k] = here * SCALE
        total = total + here
        if side == 0:
            offsets[0] = total * SCALE
            total = total + inside[...]
            offsets[1] = total * SCALE
    for k in range(copies.shape[0]):
        copies[k] = total


def final_kernel(totals, inner_sums, edge_sums, offsets, edges, _end, potential_out, end_out, potential, sems):
    copies = [
        pltpu.make_async_copy(edges.at[pl.ds(0, STEPS)], end_out.at[pl.ds(0, STEPS)], sems.at[0]),
        pltpu.make_async_copy(
            edges.at[pl.ds(STEPS, STEPS)], end_out.at[pl.ds(ROWS - STEPS, STEPS)], sems.at[1]
        ),
    ]
    for copy in copies:
        copy.start()
    here = lax.axis_index("y") * lax.axis_size("x") + lax.axis_index("x")
    total = jnp.zeros((COLS, MEMBERS), jnp.float32)
    for k in range(totals.shape[0]):
        total = total + jnp.where(k < here, totals[k], 0.0)
    total = total * SCALE
    upper = total + offsets[1]
    for k in range(STEPS):
        potential[k] = edge_sums[k] + total
        potential[ROWS - STEPS + k] = edge_sums[STEPS + k] + upper
    inner = total + offsets[0]
    piece = ROWS // FINAL_PIECES
    for part in range(FINAL_PIECES):
        for row in range(part * piece, (part + 1) * piece):
            if STEPS <= row < ROWS - STEPS:
                potential[row] = inner_sums[row - STEPS] + inner
        place = pl.ds(part * piece, piece)
        copy = pltpu.make_async_copy(potential.at[place], potential_out.at[place], sems.at[2 + part])
        copy.start()
        copies.append(copy)
    for copy in copies:
        copy.wait()


def on_device(pressure, earlier, speed_square):
    *padded, outer, inner = call(
        load_kernel,
        [PADDED] * 3 + [in_vmem(DEEP * ROWS)] * 2,
        "load",
        [pltpu.with_memory_space_constraint(a, pltpu.HBM) for a in (pressure, earlier, speed_square)],
        [HBM] * 3,
        [VMEM] * 5,
        [pltpu.SemaphoreType.DMA((3, PIECES))],
    )
    chips, ys, xs = (lax.axis_size(name) for name in ("z", "y", "x"))
    swap = lambda pairs: pairs + [(b, a) for a, b in pairs]
    outer = lax.ppermute(outer, LON, swap([(2 * z + 1, 2 * z + 2) for z in range(chips - 1)]))
    inner = lax.ppermute(inner, LON, swap([(2 * z, 2 * z + 1) for z in range(chips)]))
    same = {0: 0, 1: 1, 2: 2}
    *padded, odd, even = call(
        columns_kernel,
        [PADDED] * 3 + [in_vmem(6, WIDE)] * 2,
        "columns",
        (*padded, outer, inner),
        [VMEM] * 5,
        [VMEM] * 5,
        aliases=same,
    )
    blocks = ys * xs
    odd = lax.ppermute(odd, LAT, swap([(i, i + 1) for i in range(1, blocks - 1, 2)]))
    even = lax.ppermute(even, LAT, swap([(i, i + 1) for i in range(0, blocks, 2)]))
    *padded, end, inner_sums, inside = call(
        inner_kernel,
        [PADDED] * 3 + [WHOLE, in_vmem(INSIDE, COLS), in_vmem(COLS)],
        "inner",
        padded,
        [VMEM] * 3,
        [VMEM] * 3 + [HBM] + [VMEM] * 2,
        [in_vmem(INSIDE, COLS), pltpu.SemaphoreType.DMA],
        aliases=same,
        flops=10**8,
    )
    *_, edges, edge_sums, offsets, copies = call(
        edges_kernel,
        [PADDED] * 3 + [in_vmem(2 * STEPS, COLS)] * 2 + [in_vmem(2, COLS), in_vmem(blocks, COLS)],
        "edges",
        (*padded, odd, even, inside),
        [VMEM] * 6,
        [VMEM] * 7,
        aliases=same,
    )
    totals = lax.all_to_all(copies, LAT, 0, 0, tiled=True)
    return call(
        final_kernel,
        [WHOLE] * 2,
        "final",
        (totals, inner_sums, edge_sums, offsets, edges, end),
        [VMEM] * 5 + [HBM],
        [HBM] * 2,
        [in_vmem(ROWS, COLS), pltpu.SemaphoreType.DMA((2 + FINAL_PIECES,))],
        aliases={5: 1},
    )


def solution(mesh):
    fine = Mesh(mesh.devices.reshape(8, 4, 8, 2), ("y", "x", "z", "core"))
    spec = P(LAT, LON, None)
    return jax.shard_map(
        on_device, mesh=fine, in_specs=(spec,) * 3, out_specs=(spec,) * 2, check_vma=False
    )
```

```python
import jax
import jax.numpy as jnp
from jax import lax
from jax.experimental import pallas as pl
from jax.experimental.pallas import tpu as pltpu
from jax.sharding import Mesh, PartitionSpec as P

STEPS = 4
ROWS, COLS, MEMBERS = 32, 32, 128
PITCH = 56
LEFT = 8
HALO = STEPS
TALL = ROWS + 2 * HALO
WIDE = COLS + 2 * HALO
DEPTHS = (HALO, HALO - 1, HALO - 1)
DEEP = sum(DEPTHS)
PIECES = 4
FINAL_PIECES = 4
INSIDE = ROWS - 2 * STEPS
SCALE = 1.0 / 1024
REACHES = (3, 2, 2, 1, 2, 0)
PLACES = tuple(sum(COLS + 2 * reach for reach in REACHES[:k]) for k in range(6))
ROW_CELLS = PLACES[-1] + COLS + 2 * REACHES[-1]
LAT = ("y", "x")
LON = ("z", "core")

HBM = pl.BlockSpec(memory_space=pltpu.HBM)
VMEM = pl.BlockSpec(memory_space=pltpu.VMEM)
WHOLE = pltpu.HBM((ROWS, COLS, MEMBERS), jnp.float32)
PADDED = pltpu.VMEM((TALL, PITCH, MEMBERS), jnp.float32)


def in_vmem(*shape):
    return pltpu.VMEM((*shape, MEMBERS), jnp.float32)


def flat(ref):
    return ref.reshape(ref.shape[0] * ref.shape[1], MEMBERS)


def call(kernel, outs, name, args, specs, out_specs, scratch=(), aliases=None, flops=10**5):
    return pl.pallas_call(
        kernel,
        out_shape=outs,
        in_specs=specs,
        out_specs=out_specs,
        scratch_shapes=scratch,
        input_output_aliases=aliases or {},
        name=name,
        cost_estimate=pl.CostEstimate(flops=flops, bytes_accessed=0, transcendentals=0),
        compiler_params=pltpu.CompilerParams(vmem_limit_bytes=16 * 2**20),
    )(*args)


def cell(row, col):
    return (row + HALO) * PITCH + LEFT + col


def columns_to_message(padded, message, at_start):
    slot = 0
    for ref, depth in zip(padded, DEPTHS):
        first = jnp.where(at_start, 0, COLS - depth)
        for k in range(depth):
            message[pl.ds(slot * ROWS, ROWS), :] = flat(ref)[pl.ds(cell(0, first + k), ROWS, stride=PITCH), :]
            slot += 1


def message_to_columns(padded, message, at_start, slot=0):
    for ref, depth in zip(padded, DEPTHS):
        first = jnp.where(at_start, -depth, COLS)
        for k in range(depth):
            flat(ref)[pl.ds(cell(0, first + k), ROWS, stride=PITCH), :] = message[pl.ds(slot * ROWS, ROWS), :]
            slot += 1


def rows_to_message(padded, message, at_start):
    now, before, speed = padded
    first, second, third = (HALO + jnp.where(at_start, k, ROWS - 1 - k) for k in range(3))
    cells = slice(LEFT - HALO, LEFT - HALO + WIDE)
    beyond = speed[second, cells, :] * later_row(now, before, speed, third, LEFT - HALO, WIDE)
    values = (
        now[first, cells, :],
        now[second, cells, :] - beyond,
        before[first, cells, :] - speed[first, cells, :] * beyond,
        later_row(now, before, speed, second, LEFT - HALO, WIDE),
        speed[first, cells, :],
        speed[second, cells, :],
    )
    for value, at, reach in zip(values, PLACES, REACHES):
        message[at : at + COLS + 2 * reach] = value[HALO - reach : HALO + COLS + reach]


def message_to_rows(padded, message, at_start):
    for slot, (at, reach) in enumerate(zip(PLACES, REACHES)):
        row = HALO + jnp.where(at_start, -1 - slot % 2, ROWS + slot % 2)
        width = COLS + 2 * reach
        padded[slot // 2][row, LEFT - reach : LEFT + COLS + reach, :] = message[at : at + width]


def load_kernel(pressure, earlier, speed, *refs):
    padded, (outer, inner), sems = refs[:3], refs[3:5], refs[5]
    piece = ROWS // PIECES
    copies = [
        pltpu.make_async_copy(
            source.at[pl.ds(k * piece, piece)],
            target.at[pl.ds(HALO + k * piece, piece), pl.ds(LEFT, COLS), :],
            sems.at[i, k],
        )
        for i, (source, target) in enumerate(zip((pressure, earlier, speed), padded))
        for k in range(PIECES)
    ]
    for copy in copies:
        copy.start()
    for copy in copies:
        copy.wait()
    first_core = lax.axis_index("core") == 0
    columns_to_message(padded, outer, first_core)
    columns_to_message(padded, inner, jnp.logical_not(first_core))


def columns_kernel(_p, _e, _s, outer, inner, *refs):
    padded, (odd, even) = refs[:3], refs[3:5]
    first_core = lax.axis_index("core") == 0
    message_to_columns(padded, outer, first_core)
    message_to_columns(padded, inner, jnp.logical_not(first_core), jnp.where(first_core, DEEP, 0))
    odd_x = lax.axis_index("x") % 2 == 1
    rows_to_message(padded, odd, jnp.logical_not(odd_x))
    rows_to_message(padded, even, odd_x)
    for row in (HALO - 3, HALO + ROWS + 2):
        padded[1][row] = jnp.zeros((PITCH, MEMBERS), jnp.float32)


def later_row(source, before, speed, row, first, width):
    cells = slice(first, first + width)
    middle = source[row, cells, :]
    spread = source[row - 1, cells, :] + source[row + 1, cells, :]
    spread += source[row, first - 1 : first - 1 + width, :]
    spread += source[row, first + 1 : first + 1 + width, :]
    spread -= 4.0 * middle
    return 2.0 * middle - before[row, cells, :] + speed[row, cells, :] * spread


def set_later_row(source, before, speed, row):
    cells = slice(LEFT - HALO, LEFT - HALO + WIDE)
    before[row, cells, :] = later_row(source, before, speed, row, LEFT - HALO, WIDE)


def inner_kernel(_p, _e, _s, *refs):
    padded, (end_out, sums, total_out, end, sem) = refs[:3], refs[3:]
    now, before, speed = padded
    for step in range(1, STEPS):

        def pair(i, _, now=now, before=before, step=step):
            for k in range(2):
                set_later_row(now, before, speed, HALO + step + 2 * i + k)
            return 0

        lax.fori_loop(0, (ROWS - 2 * step) // 2, pair, 0)
        now, before = before, now

    def last(i, total):
        for k in range(2):
            row = 2 * i + k
            value = later_row(now, before, speed, row + HALO + STEPS, LEFT, COLS)
            end[row] = value
            total = total + value
            sums[row] = total * SCALE
        return total

    total_out[...] = lax.fori_loop(0, INSIDE // 2, last, jnp.zeros((COLS, MEMBERS), jnp.float32))
    copy = pltpu.make_async_copy(end, end_out.at[pl.ds(STEPS, INSIDE)], sem)
    copy.start()
    copy.wait()


def edges_kernel(_p, _e, _s, odd, even, inside, *refs):
    padded, (end, sums, offsets, copies) = refs[:3], refs[3:]
    odd_x = lax.axis_index("x") % 2 == 1
    message_to_rows(padded, odd, jnp.logical_not(odd_x))
    message_to_rows(padded, even, odd_x)
    now, before, speed = padded
    for first, count in ((-1, 2), (-2, 4), (-1, 4)):
        for k in range(count):
            set_later_row(now, before, speed, HALO + first + k)
            set_later_row(now, before, speed, HALO + ROWS - 1 - first - k)
        now, before = before, now
    total = jnp.zeros((COLS, MEMBERS), jnp.float32)
    for side in range(2):
        here = jnp.zeros((COLS, MEMBERS), jnp.float32)
        for k in range(STEPS):
            row = side * (ROWS - STEPS) + k
            value = later_row(now, before, speed, row + HALO, LEFT, COLS)
            end[side * STEPS + k] = value
            here = here + value
            sums[side * STEPS + k] = here * SCALE
        total = total + here
        if side == 0:
            offsets[0] = total * SCALE
            total = total + inside[...]
            offsets[1] = total * SCALE
    for k in range(copies.shape[0]):
        copies[k] = total


def middle_kernel(row, copies, before):
    here = lax.axis_index("x")
    total = jnp.zeros((COLS, MEMBERS), jnp.float32)
    for k in range(row.shape[0]):
        before[...] = jnp.where(k == here, total, before[...])
        total = total + row[k]
    for k in range(copies.shape[0]):
        copies[k] = total


def final_kernel(rows, before, inner_sums, edge_sums, offsets, edges, _end, potential_out, end_out, potential, sems):
    copies = [
        pltpu.make_async_copy(edges.at[pl.ds(0, STEPS)], end_out.at[pl.ds(0, STEPS)], sems.at[0]),
        pltpu.make_async_copy(
            edges.at[pl.ds(STEPS, STEPS)], end_out.at[pl.ds(ROWS - STEPS, STEPS)], sems.at[1]
        ),
    ]
    for copy in copies:
        copy.start()
    here = lax.axis_index("y")
    total = before[...]
    for k in range(rows.shape[0]):
        total = total + jnp.where(k < here, rows[k], 0.0)
    total = total * SCALE
    upper = total + offsets[1]
    for k in range(STEPS):
        potential[k] = edge_sums[k] + total
        potential[ROWS - STEPS + k] = edge_sums[STEPS + k] + upper
    inner = total + offsets[0]
    piece = ROWS // FINAL_PIECES
    for part in range(FINAL_PIECES):
        for row in range(part * piece, (part + 1) * piece):
            if STEPS <= row < ROWS - STEPS:
                potential[row] = inner_sums[row - STEPS] + inner
        place = pl.ds(part * piece, piece)
        copy = pltpu.make_async_copy(potential.at[place], potential_out.at[place], sems.at[2 + part])
        copy.start()
        copies.append(copy)
    for copy in copies:
        copy.wait()


def on_device(pressure, earlier, speed_square):
    *padded, outer, inner = call(
        load_kernel,
        [PADDED] * 3 + [in_vmem(DEEP * ROWS)] * 2,
        "load",
        [pltpu.with_memory_space_constraint(a, pltpu.HBM) for a in (pressure, earlier, speed_square)],
        [HBM] * 3,
        [VMEM] * 5,
        [pltpu.SemaphoreType.DMA((3, PIECES))],
    )
    chips, ys, xs = (lax.axis_size(name) for name in ("z", "y", "x"))
    swap = lambda pairs: pairs + [(b, a) for a, b in pairs]
    outer = lax.ppermute(outer, LON, swap([(2 * z + 1, 2 * z + 2) for z in range(chips - 1)]))
    inner = lax.all_gather(inner, "core", axis=0, tiled=True)
    same = {0: 0, 1: 1, 2: 2}
    *padded, odd, even = call(
        columns_kernel,
        [PADDED] * 3 + [in_vmem(ROW_CELLS)] * 2,
        "columns",
        (*padded, outer, inner),
        [VMEM] * 5,
        [VMEM] * 5,
        aliases=same,
    )
    blocks = ys * xs
    odd = lax.ppermute(odd, LAT, swap([(i, i + 1) for i in range(1, blocks - 1, 2)]))
    even = lax.ppermute(even, LAT, swap([(i, i + 1) for i in range(0, blocks, 2)]))
    *padded, end, inner_sums, inside = call(
        inner_kernel,
        [PADDED] * 3 + [WHOLE, in_vmem(INSIDE, COLS), in_vmem(COLS)],
        "inner",
        padded,
        [VMEM] * 3,
        [VMEM] * 3 + [HBM] + [VMEM] * 2,
        [in_vmem(INSIDE, COLS), pltpu.SemaphoreType.DMA],
        aliases=same,
        flops=10**8,
    )
    *_, edges, edge_sums, offsets, copies = call(
        edges_kernel,
        [PADDED] * 3 + [in_vmem(2 * STEPS, COLS)] * 2 + [in_vmem(2, COLS), in_vmem(xs, COLS)],
        "edges",
        (*padded, odd, even, inside),
        [VMEM] * 6,
        [VMEM] * 7,
        aliases=same,
    )
    row = lax.all_to_all(copies, "x", 0, 0, tiled=True)
    copies, before = call(
        middle_kernel,
        [in_vmem(ys, COLS), in_vmem(COLS)],
        "middle",
        (row,),
        [VMEM],
        [VMEM] * 2,
    )
    rows = lax.all_to_all(copies, "y", 0, 0, tiled=True)
    return call(
        final_kernel,
        [WHOLE] * 2,
        "final",
        (rows, before, inner_sums, edge_sums, offsets, edges, end),
        [VMEM] * 6 + [HBM],
        [HBM] * 2,
        [in_vmem(ROWS, COLS), pltpu.SemaphoreType.DMA((2 + FINAL_PIECES,))],
        aliases={6: 1},
    )


def solution(mesh):
    fine = Mesh(mesh.devices.reshape(8, 4, 8, 2), ("y", "x", "z", "core"))
    spec = P(LAT, LON, None)
    return jax.shard_map(
        on_device, mesh=fine, in_specs=(spec,) * 3, out_specs=(spec,) * 2, check_vma=False
    )
```

```python
import jax
import jax.numpy as jnp
from jax import lax
from jax.experimental import pallas as pl
from jax.experimental.pallas import tpu as pltpu
from jax.sharding import Mesh, PartitionSpec as P

STEPS = 4
ROWS, COLS, MEMBERS = 32, 32, 128
PITCH = 56
LEFT = 8
HALO = STEPS
TALL = ROWS + 2 * HALO
WIDE = COLS + 2 * HALO
DEPTHS = (HALO, HALO - 1, HALO - 1)
DEEP = sum(DEPTHS)
TILE = 8
FINAL_PIECES = 4
INSIDE = ROWS - 2 * STEPS
SCALE = 1.0 / 1024
REACHES = (3, 2, 2, 1, 2, 0)
PLACES = tuple(sum(COLS + 2 * reach for reach in REACHES[:k]) for k in range(6))
ROW_CELLS = PLACES[-1] + COLS + 2 * REACHES[-1]
LAT = ("y", "x")
LON = ("z", "core")

HBM = pl.BlockSpec(memory_space=pltpu.HBM)
VMEM = pl.BlockSpec(memory_space=pltpu.VMEM)
WHOLE = pltpu.HBM((ROWS, COLS, MEMBERS), jnp.float32)
PADDED = pltpu.VMEM((TALL, PITCH, MEMBERS), jnp.float32)


def in_vmem(*shape):
    return pltpu.VMEM((*shape, MEMBERS), jnp.float32)


def flat(ref):
    return ref.reshape(ref.shape[0] * ref.shape[1], MEMBERS)


def call(kernel, outs, name, args, specs, out_specs, scratch=(), aliases=None, flops=10**5):
    return pl.pallas_call(
        kernel,
        out_shape=outs,
        in_specs=specs,
        out_specs=out_specs,
        scratch_shapes=scratch,
        input_output_aliases=aliases or {},
        name=name,
        cost_estimate=pl.CostEstimate(flops=flops, bytes_accessed=0, transcendentals=0),
        compiler_params=pltpu.CompilerParams(vmem_limit_bytes=16 * 2**20),
    )(*args)


def cell(row, col):
    return (row + HALO) * PITCH + LEFT + col


def columns_to_message(padded, message, at_start):
    slot = 0
    for ref, depth in zip(padded, DEPTHS):
        first = jnp.where(at_start, 0, COLS - depth)
        for k in range(depth):
            message[pl.ds(slot * ROWS, ROWS), :] = flat(ref)[pl.ds(cell(0, first + k), ROWS, stride=PITCH), :]
            slot += 1


def message_to_columns(padded, message, at_start, slot=0):
    for ref, depth in zip(padded, DEPTHS):
        first = jnp.where(at_start, -depth, COLS)
        for k in range(depth):
            flat(ref)[pl.ds(cell(0, first + k), ROWS, stride=PITCH), :] = message[pl.ds(slot * ROWS, ROWS), :]
            slot += 1


def rows_to_message(padded, message, at_start):
    now, before, speed = padded
    first, second, third = (HALO + jnp.where(at_start, k, ROWS - 1 - k) for k in range(3))
    cells = slice(LEFT - HALO, LEFT - HALO + WIDE)
    beyond = speed[second, cells, :] * later_row(now, before, speed, third, LEFT - HALO, WIDE)
    values = (
        now[first, cells, :],
        now[second, cells, :] - beyond,
        before[first, cells, :] - speed[first, cells, :] * beyond,
        later_row(now, before, speed, second, LEFT - HALO, WIDE),
        speed[first, cells, :],
        speed[second, cells, :],
    )
    for value, at, reach in zip(values, PLACES, REACHES):
        message[at : at + COLS + 2 * reach] = value[HALO - reach : HALO + COLS + reach]


def message_to_rows(padded, message, at_start):
    for slot, (at, reach) in enumerate(zip(PLACES, REACHES)):
        row = HALO + jnp.where(at_start, -1 - slot % 2, ROWS + slot % 2)
        width = COLS + 2 * reach
        padded[slot // 2][row, LEFT - reach : LEFT + COLS + reach, :] = message[at : at + width]


def outer_kernel(pressure, earlier, speed, message, tiles, sems):
    first_core = lax.axis_index("core") == 0
    first = pl.multiple_of(jnp.where(first_core, 0, COLS - TILE), TILE)
    copies = [
        pltpu.make_async_copy(source.at[:, pl.ds(first, TILE), :], tiles.at[i], sems.at[i])
        for i, source in enumerate((pressure, earlier, speed))
    ]
    for copy in copies:
        copy.start()
    slot = 0
    for i, depth in enumerate(DEPTHS):
        copies[i].wait()
        cells = tiles.at[i].reshape(ROWS * TILE, MEMBERS)
        start = jnp.where(first_core, 0, TILE - depth)
        for k in range(depth):
            message[pl.ds(slot * ROWS, ROWS), :] = cells[pl.ds(start + k, ROWS, stride=TILE), :]
            slot += 1


def load_kernel(pressure, earlier, speed, *refs):
    padded, inner = refs[:3], refs[3]
    for source, target in zip((pressure, earlier, speed), padded):

        def some(i, _, source=source, target=target):
            for k in range(4):
                target[HALO + 4 * i + k, LEFT : LEFT + COLS, :] = source[4 * i + k]
            return 0

        lax.fori_loop(0, ROWS // 4, some, 0)
    columns_to_message(padded, inner, lax.axis_index("core") != 0)


def columns_kernel(_p, _e, _s, outer, inner, *refs):
    padded, (odd, even) = refs[:3], refs[3:5]
    first_core = lax.axis_index("core") == 0
    message_to_columns(padded, outer, first_core)
    message_to_columns(padded, inner, jnp.logical_not(first_core), jnp.where(first_core, DEEP, 0))
    odd_x = lax.axis_index("x") % 2 == 1
    rows_to_message(padded, odd, jnp.logical_not(odd_x))
    rows_to_message(padded, even, odd_x)
    for row in (HALO - 3, HALO + ROWS + 2):
        padded[1][row] = jnp.zeros((PITCH, MEMBERS), jnp.float32)


def later_row(source, before, speed, row, first, width):
    cells = slice(first, first + width)
    middle = source[row, cells, :]
    spread = source[row - 1, cells, :] + source[row + 1, cells, :]
    spread += source[row, first - 1 : first - 1 + width, :]
    spread += source[row, first + 1 : first + 1 + width, :]
    spread -= 4.0 * middle
    return 2.0 * middle - before[row, cells, :] + speed[row, cells, :] * spread


def set_later_row(source, before, speed, row):
    cells = slice(LEFT - HALO, LEFT - HALO + WIDE)
    before[row, cells, :] = later_row(source, before, speed, row, LEFT - HALO, WIDE)


def inner_kernel(_p, _e, _s, *refs):
    padded, (end_out, sums, total_out, end, sem) = refs[:3], refs[3:]
    now, before, speed = padded
    for step in range(1, STEPS):

        def pair(i, _, now=now, before=before, step=step):
            for k in range(2):
                set_later_row(now, before, speed, HALO + step + 2 * i + k)
            return 0

        lax.fori_loop(0, (ROWS - 2 * step) // 2, pair, 0)
        now, before = before, now

    def last(i, total):
        for k in range(2):
            row = 2 * i + k
            value = later_row(now, before, speed, row + HALO + STEPS, LEFT, COLS)
            end[row] = value
            total = total + value
            sums[row] = total * SCALE
        return total

    total_out[...] = lax.fori_loop(0, INSIDE // 2, last, jnp.zeros((COLS, MEMBERS), jnp.float32))
    copy = pltpu.make_async_copy(end, end_out.at[pl.ds(STEPS, INSIDE)], sem)
    copy.start()
    copy.wait()


def edges_kernel(_p, _e, _s, odd, even, inside, *refs):
    padded, (end, sums, offsets, copies) = refs[:3], refs[3:]
    odd_x = lax.axis_index("x") % 2 == 1
    message_to_rows(padded, odd, jnp.logical_not(odd_x))
    message_to_rows(padded, even, odd_x)
    now, before, speed = padded
    for first, count in ((-1, 2), (-2, 4), (-1, 4)):
        for k in range(count):
            set_later_row(now, before, speed, HALO + first + k)
            set_later_row(now, before, speed, HALO + ROWS - 1 - first - k)
        now, before = before, now
    total = jnp.zeros((COLS, MEMBERS), jnp.float32)
    for side in range(2):
        here = jnp.zeros((COLS, MEMBERS), jnp.float32)
        for k in range(STEPS):
            row = side * (ROWS - STEPS) + k
            value = later_row(now, before, speed, row + HALO, LEFT, COLS)
            end[side * STEPS + k] = value
            here = here + value
            sums[side * STEPS + k] = here * SCALE
        total = total + here
        if side == 0:
            offsets[0] = total * SCALE
            total = total + inside[...]
            offsets[1] = total * SCALE
    for k in range(copies.shape[0]):
        copies[k] = total


def middle_kernel(row, copies, before):
    here = lax.axis_index("x")
    total = jnp.zeros((COLS, MEMBERS), jnp.float32)
    for k in range(row.shape[0]):
        before[...] = jnp.where(k == here, total, before[...])
        total = total + row[k]
    for k in range(copies.shape[0]):
        copies[k] = total


def final_kernel(rows, before, inner_sums, edge_sums, offsets, edges, _end, potential_out, end_out, potential, sems):
    copies = [
        pltpu.make_async_copy(edges.at[pl.ds(0, STEPS)], end_out.at[pl.ds(0, STEPS)], sems.at[0]),
        pltpu.make_async_copy(
            edges.at[pl.ds(STEPS, STEPS)], end_out.at[pl.ds(ROWS - STEPS, STEPS)], sems.at[1]
        ),
    ]
    for copy in copies:
        copy.start()
    here = lax.axis_index("y")
    total = before[...]
    for k in range(rows.shape[0]):
        total = total + jnp.where(k < here, rows[k], 0.0)
    total = total * SCALE
    upper = total + offsets[1]
    for k in range(STEPS):
        potential[k] = edge_sums[k] + total
        potential[ROWS - STEPS + k] = edge_sums[STEPS + k] + upper
    inner = total + offsets[0]
    piece = ROWS // FINAL_PIECES
    for part in range(FINAL_PIECES):
        for row in range(part * piece, (part + 1) * piece):
            if STEPS <= row < ROWS - STEPS:
                potential[row] = inner_sums[row - STEPS] + inner
        place = pl.ds(part * piece, piece)
        copy = pltpu.make_async_copy(potential.at[place], potential_out.at[place], sems.at[2 + part])
        copy.start()
        copies.append(copy)
    for copy in copies:
        copy.wait()


def on_device(pressure, earlier, speed_square):
    args = [pltpu.with_memory_space_constraint(a, pltpu.HBM) for a in (pressure, earlier, speed_square)]
    outer = call(
        outer_kernel,
        in_vmem(DEEP * ROWS),
        "outer",
        args,
        [HBM] * 3,
        VMEM,
        [in_vmem(3, ROWS, TILE), pltpu.SemaphoreType.DMA((3,))],
    )
    chips, ys, xs = (lax.axis_size(name) for name in ("z", "y", "x"))
    swap = lambda pairs: pairs + [(b, a) for a, b in pairs]
    outer = lax.ppermute(outer, LON, swap([(2 * z + 1, 2 * z + 2) for z in range(chips - 1)]))
    *padded, inner = call(
        load_kernel,
        [PADDED] * 3 + [in_vmem(DEEP * ROWS)],
        "load",
        [pltpu.with_memory_space_constraint(a, pltpu.VMEM) for a in (pressure, earlier, speed_square)],
        [VMEM] * 3,
        [VMEM] * 4,
    )
    inner = lax.all_gather(inner, "core", axis=0, tiled=True)
    same = {0: 0, 1: 1, 2: 2}
    *padded, odd, even = call(
        columns_kernel,
        [PADDED] * 3 + [in_vmem(ROW_CELLS)] * 2,
        "columns",
        (*padded, outer, inner),
        [VMEM] * 5,
        [VMEM] * 5,
        aliases=same,
    )
    blocks = ys * xs
    odd = lax.ppermute(odd, LAT, swap([(i, i + 1) for i in range(1, blocks - 1, 2)]))
    even = lax.ppermute(even, LAT, swap([(i, i + 1) for i in range(0, blocks, 2)]))
    *padded, end, inner_sums, inside = call(
        inner_kernel,
        [PADDED] * 3 + [WHOLE, in_vmem(INSIDE, COLS), in_vmem(COLS)],
        "inner",
        padded,
        [VMEM] * 3,
        [VMEM] * 3 + [HBM] + [VMEM] * 2,
        [in_vmem(INSIDE, COLS), pltpu.SemaphoreType.DMA],
        aliases=same,
        flops=10**8,
    )
    *_, edges, edge_sums, offsets, copies = call(
        edges_kernel,
        [PADDED] * 3 + [in_vmem(2 * STEPS, COLS)] * 2 + [in_vmem(2, COLS), in_vmem(xs, COLS)],
        "edges",
        (*padded, odd, even, inside),
        [VMEM] * 6,
        [VMEM] * 7,
        aliases=same,
    )
    row = lax.all_to_all(copies, "x", 0, 0, tiled=True)
    copies, before = call(
        middle_kernel,
        [in_vmem(ys, COLS), in_vmem(COLS)],
        "middle",
        (row,),
        [VMEM],
        [VMEM] * 2,
    )
    rows = lax.all_to_all(copies, "y", 0, 0, tiled=True)
    return call(
        final_kernel,
        [WHOLE] * 2,
        "final",
        (rows, before, inner_sums, edge_sums, offsets, edges, end),
        [VMEM] * 6 + [HBM],
        [HBM] * 2,
        [in_vmem(ROWS, COLS), pltpu.SemaphoreType.DMA((2 + FINAL_PIECES,))],
        aliases={6: 1},
    )


def solution(mesh):
    fine = Mesh(mesh.devices.reshape(8, 4, 8, 2), ("y", "x", "z", "core"))
    spec = P(LAT, LON, None)
    return jax.shard_map(
        on_device, mesh=fine, in_specs=(spec,) * 3, out_specs=(spec,) * 2, check_vma=False
    )
```

```python
import jax
import jax.numpy as jnp
from jax import lax
from jax.experimental import pallas as pl
from jax.experimental.pallas import tpu as pltpu
from jax.sharding import Mesh, PartitionSpec as P

STEPS = 4
ROWS, COLS, MEMBERS = 32, 32, 128
PITCH = 56
LEFT = 8
HALO = STEPS
TALL = ROWS + 2 * HALO
WIDE = COLS + 2 * HALO
DEPTHS = (HALO, HALO - 1, HALO - 1)
DEEP = sum(DEPTHS)
TILE = 8
FINAL_PIECES = 4
INSIDE = ROWS - 2 * STEPS
SCALE = 1.0 / 1024
REACHES = (3, 2, 2, 1, 2, 0)
PLACES = tuple(sum(COLS + 2 * reach for reach in REACHES[:k]) for k in range(6))
ROW_CELLS = -(-(PLACES[-1] + COLS + 2 * REACHES[-1]) // 8) * 8
X = ("xh", "xl")
LAT = ("y", *X)
LON = ("z", "core")

HBM = pl.BlockSpec(memory_space=pltpu.HBM)
VMEM = pl.BlockSpec(memory_space=pltpu.VMEM)
WHOLE = pltpu.HBM((ROWS, COLS, MEMBERS), jnp.float32)
PADDED = pltpu.VMEM((TALL, PITCH, MEMBERS), jnp.float32)
RAW = pltpu.VMEM((2 * HALO, PITCH, MEMBERS), jnp.float32)


def in_vmem(*shape):
    return pltpu.VMEM((*shape, MEMBERS), jnp.float32)


def flat(ref):
    return ref.reshape(ref.shape[0] * ref.shape[1], MEMBERS)


def call(kernel, outs, name, args, specs, out_specs, scratch=(), aliases=None, flops=10**5):
    return pl.pallas_call(
        kernel,
        out_shape=outs,
        in_specs=specs,
        out_specs=out_specs,
        scratch_shapes=scratch,
        input_output_aliases=aliases or {},
        name=name,
        cost_estimate=pl.CostEstimate(flops=flops, bytes_accessed=0, transcendentals=0),
        compiler_params=pltpu.CompilerParams(vmem_limit_bytes=16 * 2**20),
    )(*args)


def cell(row, col):
    return (row + HALO) * PITCH + LEFT + col


def columns_to_message(padded, message, at_start):
    slot = 0
    for ref, depth in zip(padded, DEPTHS):
        first = jnp.where(at_start, 0, COLS - depth)
        for k in range(depth):
            message[pl.ds(slot * ROWS, ROWS), :] = flat(ref)[pl.ds(cell(0, first + k), ROWS, stride=PITCH), :]
            slot += 1


def message_to_columns(padded, raw, message, at_start, slot=0):
    for ref, ends, depth in zip(padded, raw, DEPTHS):
        first = jnp.where(at_start, -depth, COLS)
        for k in range(depth):
            at = slot * ROWS
            flat(ref)[pl.ds(cell(0, first + k), ROWS, stride=PITCH), :] = message[pl.ds(at, ROWS), :]
            for row, source in ((0, at), (HALO, at + ROWS - HALO)):
                place = pl.ds(row * PITCH + LEFT + first + k, HALO, stride=PITCH)
                flat(ends)[place, :] = message[pl.ds(source, HALO), :]
            slot += 1


def rows_to_message(raw, message, at_start):
    now, before, speed = raw
    first, second, third = (jnp.where(at_start, k, 2 * HALO - 1 - k) for k in range(3))
    cells = slice(LEFT - HALO, LEFT - HALO + WIDE)
    beyond = speed[second, cells, :] * later_row(now, before, speed, third, LEFT - HALO, WIDE)
    values = (
        now[first, cells, :],
        now[second, cells, :] - beyond,
        before[first, cells, :] - speed[first, cells, :] * beyond,
        later_row(now, before, speed, second, LEFT - HALO, WIDE),
        speed[first, cells, :],
        speed[second, cells, :],
    )
    for value, at, reach in zip(values, PLACES, REACHES):
        message[at : at + COLS + 2 * reach] = value[HALO - reach : HALO + COLS + reach]


def message_to_rows(padded, message, at_start, place=0):
    for slot, (at, reach) in enumerate(zip(PLACES, REACHES)):
        row = HALO + jnp.where(at_start, -1 - slot % 2, ROWS + slot % 2)
        width = COLS + 2 * reach
        padded[slot // 2][row, LEFT - reach : LEFT + COLS + reach, :] = message[pl.ds(place + at, width), :]


def outer_kernel(pressure, earlier, speed, message, tiles, sems):
    first_core = lax.axis_index("core") == 0
    first = pl.multiple_of(jnp.where(first_core, 0, COLS - TILE), TILE)
    copies = [
        pltpu.make_async_copy(source.at[:, pl.ds(first, TILE), :], tiles.at[i], sems.at[i])
        for i, source in enumerate((pressure, earlier, speed))
    ]
    for copy in copies:
        copy.start()
    slot = 0
    for i, depth in enumerate(DEPTHS):
        copies[i].wait()
        cells = tiles.at[i].reshape(ROWS * TILE, MEMBERS)
        start = jnp.where(first_core, 0, TILE - depth)
        for k in range(depth):
            message[pl.ds(slot * ROWS, ROWS), :] = cells[pl.ds(start + k, ROWS, stride=TILE), :]
            slot += 1


def load_kernel(pressure, earlier, speed, *refs):
    padded, raw, inner = refs[:3], refs[3:6], refs[6]
    for source, target, ends in zip((pressure, earlier, speed), padded, raw):
        for k in range(HALO):
            ends[k, LEFT : LEFT + COLS, :] = source[k]
            ends[HALO + k, LEFT : LEFT + COLS, :] = source[ROWS - HALO + k]

        def some(i, _, source=source, target=target):
            for k in range(4):
                target[HALO + 4 * i + k, LEFT : LEFT + COLS, :] = source[4 * i + k]
            return 0

        lax.fori_loop(0, ROWS // 4, some, 0)
    columns_to_message(padded, inner, lax.axis_index("core") != 0)


def columns_kernel(*refs):
    outer, inner = refs[6:8]
    padded, raw, (odd, even) = refs[8:11], refs[11:14], refs[14:16]
    first_core = lax.axis_index("core") == 0
    message_to_columns(padded, raw, outer, first_core)
    message_to_columns(padded, raw, inner, jnp.logical_not(first_core), jnp.where(first_core, DEEP, 0))
    odd_x = lax.axis_index(X) % 2 == 1
    rows_to_message(raw, odd, jnp.logical_not(odd_x))
    rows_to_message(raw, even, odd_x)
    for row in (HALO - 3, HALO + ROWS + 2):
        padded[1][row] = jnp.zeros((PITCH, MEMBERS), jnp.float32)


def later_row(source, before, speed, row, first, width):
    cells = slice(first, first + width)
    middle = source[row, cells, :]
    spread = source[row - 1, cells, :] + source[row + 1, cells, :]
    spread += source[row, first - 1 : first - 1 + width, :]
    spread += source[row, first + 1 : first + 1 + width, :]
    spread -= 4.0 * middle
    return 2.0 * middle - before[row, cells, :] + speed[row, cells, :] * spread


def set_later_row(source, before, speed, row, first=-HALO, width=WIDE):
    cells = slice(LEFT + first, LEFT + first + width)
    before[row, cells, :] = later_row(source, before, speed, row, LEFT + first, width)


def own_steps(padded, end, sums, inside):
    now, before, speed = padded
    for step in range(1, STEPS):

        def pair(i, _, now=now, before=before, step=step):
            for k in range(2):
                row = HALO + step + 2 * i + k
                set_later_row(now, before, speed, row, step, COLS - 2 * step)
            return 0

        lax.fori_loop(0, (ROWS - 2 * step) // 2, pair, 0)
        now, before = before, now
    cells = slice(STEPS, COLS - STEPS)

    def last(i, total):
        for k in range(2):
            row = STEPS + 2 * i + k
            value = later_row(now, before, speed, row + HALO, LEFT + STEPS, COLS - 2 * STEPS)
            end[row, cells, :] = value
            total = total + value
            sums[row, cells, :] = total * SCALE
        return total

    zero = jnp.zeros((COLS - 2 * STEPS, MEMBERS), jnp.float32)
    inside[cells, :] = lax.fori_loop(0, INSIDE // 2, last, zero)


def first_core_kernel(_p, _e, _s, _message, *refs):
    @pl.when(lax.axis_index("core") == 0)
    def _():
        own_steps(refs[:3], *refs[4:])


def second_core_kernel(_p, _e, _s, _end, _sums, _inside, _message, *refs):
    @pl.when(lax.axis_index("core") != 0)
    def _():
        own_steps(refs[:3], *refs[3:])


def edges_kernel(_p, _e, _s, odd, even, _end, _sums, _inside, *refs):
    padded, (end, sums, inside, offsets, copies) = refs[:3], refs[3:]
    now, before, speed = padded
    for step in range(1, STEPS):
        for row in range(step, ROWS - step):
            for first in (step - STEPS, COLS - step):
                set_later_row(now, before, speed, row + HALO, first, STEPS)
        now, before = before, now
    for first in (0, COLS - STEPS):
        cells = slice(first, first + STEPS)
        total = jnp.zeros((STEPS, MEMBERS), jnp.float32)
        for row in range(STEPS, ROWS - STEPS):
            value = later_row(now, before, speed, row + HALO, LEFT + first, STEPS)
            end[row, cells, :] = value
            total = total + value
            sums[row, cells, :] = total * SCALE
        inside[cells, :] = total

    odd_x = lax.axis_index(X) % 2 == 1
    message_to_rows(padded, odd, jnp.logical_not(odd_x))
    message_to_rows(padded, even, odd_x, jnp.where(odd_x, 0, ROW_CELLS))
    now, before, speed = padded
    for first, count in ((-1, 2), (-2, 4), (-1, 4)):
        for k in range(count):
            set_later_row(now, before, speed, HALO + first + k)
            set_later_row(now, before, speed, HALO + ROWS - 1 - first - k)
        now, before = before, now
    total = jnp.zeros((COLS, MEMBERS), jnp.float32)
    for side in range(2):
        here = jnp.zeros((COLS, MEMBERS), jnp.float32)
        for k in range(STEPS):
            row = side * (ROWS - STEPS) + k
            value = later_row(now, before, speed, row + HALO, LEFT, COLS)
            end[row] = value
            here = here + value
            sums[row] = here * SCALE
        total = total + here
        if side == 0:
            offsets[0] = total * SCALE
            total = total + inside[...]
            offsets[1] = total * SCALE
    for k in range(copies.shape[0]):
        copies[k] = total


def middle_kernel(row, copies, before):
    here = lax.axis_index(X)
    total = jnp.zeros((COLS, MEMBERS), jnp.float32)
    for k in range(row.shape[0]):
        before[...] = jnp.where(k == here, total, before[...])
        total = total + row[k]
    for k in range(copies.shape[0]):
        copies[k] = total


def final_kernel(rows, before, sums, offsets, end, potential_out, end_out, potential, sems):
    copies = [pltpu.make_async_copy(end, end_out, sems.at[FINAL_PIECES])]
    copies[0].start()
    here = lax.axis_index("y")
    total = before[...]
    for k in range(rows.shape[0]):
        total = total + jnp.where(k < here, rows[k], 0.0)
    total = total * SCALE
    inner = total + offsets[0]
    upper = total + offsets[1]
    piece = ROWS // FINAL_PIECES
    for part in range(FINAL_PIECES):
        for row in range(part * piece, (part + 1) * piece):
            below = total if row < STEPS else inner if row < ROWS - STEPS else upper
            potential[row] = sums[row] + below
        place = pl.ds(part * piece, piece)
        copy = pltpu.make_async_copy(potential.at[place], potential_out.at[place], sems.at[part])
        copy.start()
        copies.append(copy)
    for copy in copies:
        copy.wait()


def on_device(pressure, earlier, speed_square):
    args = [pltpu.with_memory_space_constraint(a, pltpu.HBM) for a in (pressure, earlier, speed_square)]
    outer = call(
        outer_kernel,
        in_vmem(DEEP * ROWS),
        "outer",
        args,
        [HBM] * 3,
        VMEM,
        [in_vmem(3, ROWS, TILE), pltpu.SemaphoreType.DMA((3,))],
    )
    chips, ys, xs = (lax.axis_size(name) for name in ("z", "y", X))
    swap = lambda pairs: pairs + [(b, a) for a, b in pairs]
    outer = lax.ppermute(outer, LON, swap([(2 * z + 1, 2 * z + 2) for z in range(chips - 1)]))
    *padded, inner = call(
        load_kernel,
        [PADDED] * 3 + [RAW] * 3 + [in_vmem(DEEP * ROWS)],
        "load",
        [pltpu.with_memory_space_constraint(a, pltpu.VMEM) for a in (pressure, earlier, speed_square)],
        [VMEM] * 3,
        [VMEM] * 7,
    )
    padded, raw = padded[:3], padded[3:]
    same = {0: 0, 1: 1, 2: 2}
    *padded, inner, end, sums, inside = call(
        first_core_kernel,
        [PADDED] * 3 + [in_vmem(DEEP * ROWS)] + [in_vmem(ROWS, COLS)] * 2 + [in_vmem(COLS)],
        "own0",
        (*padded, inner),
        [VMEM] * 4,
        [VMEM] * 7,
        aliases={**same, 3: 3},
    )
    inner = lax.all_gather(inner, "core", axis=0, tiled=True)
    *padded, end, sums, inside = call(
        second_core_kernel,
        [PADDED] * 3 + [in_vmem(ROWS, COLS)] * 2 + [in_vmem(COLS)],
        "own1",
        (*padded, end, sums, inside, inner),
        [VMEM] * 7,
        [VMEM] * 6,
        aliases={k: k for k in range(6)},
        flops=10**8,
    )
    *padded, odd, even = call(
        columns_kernel,
        [PADDED] * 3 + [RAW] * 3 + [in_vmem(ROW_CELLS)] * 2,
        "columns",
        (*padded, *raw, outer, inner),
        [VMEM] * 8,
        [VMEM] * 8,
        aliases={k: k for k in range(6)},
    )
    padded = padded[:3]
    blocks = ys * xs
    odd = lax.ppermute(odd, LAT, swap([(i, i + 1) for i in range(1, blocks - 1, 2)]))
    even = lax.all_gather(even, "xl", axis=0, tiled=True)
    *_, end, sums, _, offsets, copies = call(
        edges_kernel,
        [PADDED] * 3 + [in_vmem(ROWS, COLS)] * 2 + [in_vmem(COLS), in_vmem(2, COLS), in_vmem(xs, COLS)],
        "edges",
        (*padded, odd, even, end, sums, inside),
        [VMEM] * 8,
        [VMEM] * 8,
        aliases={**same, 5: 3, 6: 4, 7: 5},
    )
    row = lax.all_to_all(copies, X, 0, 0, tiled=True)
    copies, before = call(
        middle_kernel,
        [in_vmem(ys, COLS), in_vmem(COLS)],
        "middle",
        (row,),
        [VMEM],
        [VMEM] * 2,
    )
    rows = lax.all_to_all(copies, "y", 0, 0, tiled=True)
    return call(
        final_kernel,
        [WHOLE] * 2,
        "final",
        (rows, before, sums, offsets, end),
        [VMEM] * 5,
        [HBM] * 2,
        [in_vmem(ROWS, COLS), pltpu.SemaphoreType.DMA((FINAL_PIECES + 1,))],
    )


def solution(mesh):
    fine = Mesh(mesh.devices.reshape(8, 2, 2, 8, 2), ("y", *X, "z", "core"))
    spec = P(LAT, LON, None)
    return jax.shard_map(
        on_device, mesh=fine, in_specs=(spec,) * 3, out_specs=(spec,) * 2, check_vma=False
    )
```

```python
import jax
import jax.numpy as jnp
from jax import lax
from jax.experimental import pallas as pl
from jax.experimental.pallas import tpu as pltpu
from jax.sharding import Mesh, PartitionSpec as P

STEPS = 4
ROWS, COLS, MEMBERS = 32, 32, 128
PITCH = 56
LEFT = 8
HALO = STEPS
TALL = ROWS + 2 * HALO
WIDE = COLS + 2 * HALO
DEPTHS = (HALO, HALO - 1, HALO - 1)
DEEP = sum(DEPTHS)
TILE = 8
FINAL_PIECES = 4
INSIDE = ROWS - 2 * STEPS
SCALE = 1.0 / 1024
REACHES = (3, 2, 2, 1, 2, 0)
PLACES = tuple(sum(COLS + 2 * reach for reach in REACHES[:k]) for k in range(6))
ROW_CELLS = -(-(PLACES[-1] + COLS + 2 * REACHES[-1]) // 8) * 8
X = ("xh", "xl")
LAT = ("y", *X)
LON = ("z", "core")

HBM = pl.BlockSpec(memory_space=pltpu.HBM)
VMEM = pl.BlockSpec(memory_space=pltpu.VMEM)
WHOLE = pltpu.HBM((ROWS, COLS, MEMBERS), jnp.float32)
PADDED = pltpu.VMEM((TALL, PITCH, MEMBERS), jnp.float32)
RAW = pltpu.VMEM((3 * HALO, PITCH, MEMBERS), jnp.float32)


def in_vmem(*shape):
    return pltpu.VMEM((*shape, MEMBERS), jnp.float32)


def flat(ref):
    return ref.reshape(ref.shape[0] * ref.shape[1], MEMBERS)


def call(kernel, outs, name, args, specs, out_specs, scratch=(), aliases=None, flops=10**5):
    return pl.pallas_call(
        kernel,
        out_shape=outs,
        in_specs=specs,
        out_specs=out_specs,
        scratch_shapes=scratch,
        input_output_aliases=aliases or {},
        name=name,
        cost_estimate=pl.CostEstimate(flops=flops, bytes_accessed=0, transcendentals=0),
        compiler_params=pltpu.CompilerParams(vmem_limit_bytes=16 * 2**20),
    )(*args)


def cell(row, col):
    return (row + HALO) * PITCH + LEFT + col


def columns_to_message(padded, message, at_start):
    slot = 0
    for ref, depth in zip(padded, DEPTHS):
        first = jnp.where(at_start, 0, COLS - depth)
        for k in range(depth):
            message[pl.ds(slot * ROWS, ROWS), :] = flat(ref)[pl.ds(cell(0, first + k), ROWS, stride=PITCH), :]
            slot += 1


def message_to_columns(padded, raw, message, at_start, slot=0):
    for ref, ends, depth in zip(padded, raw, DEPTHS):
        first = jnp.where(at_start, -depth, COLS)
        for k in range(depth):
            at = slot * ROWS
            flat(ref)[pl.ds(cell(0, first + k), ROWS, stride=PITCH), :] = message[pl.ds(at, ROWS), :]
            first_rows = message[pl.ds(at, 2 * HALO), :][:HALO]
            last_rows = message[pl.ds(at + ROWS - 2 * HALO, 2 * HALO), :][HALO:]
            for row, values in ((0, first_rows), (HALO, last_rows)):
                place = pl.ds(row * PITCH + LEFT + first + k, HALO, stride=PITCH)
                flat(ends)[place, :] = values
            slot += 1


def rows_to_message(raw, message, at_start):
    now, before, speed = raw
    first, second, third = (jnp.where(at_start, k, 2 * HALO - 1 - k) for k in range(3))
    cells = slice(LEFT - HALO, LEFT - HALO + WIDE)
    beyond = speed[second, cells, :] * later_row(now, before, speed, third, LEFT - HALO, WIDE)
    values = (
        now[first, cells, :],
        now[second, cells, :] - beyond,
        before[first, cells, :] - speed[first, cells, :] * beyond,
        later_row(now, before, speed, second, LEFT - HALO, WIDE),
        speed[first, cells, :],
        speed[second, cells, :],
    )
    for value, at, reach in zip(values, PLACES, REACHES):
        message[at : at + COLS + 2 * reach] = value[HALO - reach : HALO + COLS + reach]


def message_to_rows(padded, message, at_start, place=0):
    for slot, (at, reach) in enumerate(zip(PLACES, REACHES)):
        row = HALO + jnp.where(at_start, -1 - slot % 2, ROWS + slot % 2)
        width = COLS + 2 * reach
        padded[slot // 2][row, LEFT - reach : LEFT + COLS + reach, :] = message[pl.ds(place + at, width), :]


def outer_kernel(pressure, earlier, speed, message, tiles, sems):
    first_core = lax.axis_index("core") == 0
    first = pl.multiple_of(jnp.where(first_core, 0, COLS - TILE), TILE)
    copies = [
        pltpu.make_async_copy(source.at[:, pl.ds(first, TILE), :], tiles.at[i, pl.ds(0, ROWS)], sems.at[i])
        for i, source in enumerate((pressure, earlier, speed))
    ]
    for copy in copies:
        copy.start()
    slot = 0
    for i, depth in enumerate(DEPTHS):
        copies[i].wait()
        cells = tiles.at[i].reshape((ROWS + 1) * TILE, MEMBERS)
        start = jnp.where(first_core, 0, TILE - depth)
        for k in range(depth):
            message[pl.ds(slot * ROWS, ROWS), :] = cells[pl.ds(start + k, ROWS, stride=TILE), :]
            slot += 1


def load_kernel(pressure, earlier, speed, *refs):
    padded, raw, inner = refs[:3], refs[3:6], refs[6]
    for source, target, ends in zip((pressure, earlier, speed), padded, raw):
        for k in range(HALO):
            ends[k, LEFT : LEFT + COLS, :] = source[k]
            ends[HALO + k, LEFT : LEFT + COLS, :] = source[ROWS - HALO + k]

        def some(i, _, source=source, target=target):
            for k in range(4):
                target[HALO + 4 * i + k, LEFT : LEFT + COLS, :] = source[4 * i + k]
            return 0

        lax.fori_loop(0, ROWS // 4, some, 0)
    columns_to_message(padded, inner, lax.axis_index("core") != 0)


def columns_kernel(*refs):
    outer, inner = refs[6:8]
    padded, raw, (odd, even) = refs[8:11], refs[11:14], refs[14:16]
    first_core = lax.axis_index("core") == 0
    message_to_columns(padded, raw, outer, first_core)
    message_to_columns(padded, raw, inner, jnp.logical_not(first_core), jnp.where(first_core, DEEP, 0))
    odd_x = lax.axis_index(X) % 2 == 1
    rows_to_message(raw, odd, jnp.logical_not(odd_x))
    rows_to_message(raw, even, odd_x)
    for row in (HALO - 3, HALO + ROWS + 2):
        padded[1][row] = jnp.zeros((PITCH, MEMBERS), jnp.float32)


def later_row(source, before, speed, row, first, width):
    cells = slice(first, first + width)
    middle = source[row, cells, :]
    spread = source[row - 1, cells, :] + source[row + 1, cells, :]
    spread += source[row, first - 1 : first - 1 + width, :]
    spread += source[row, first + 1 : first + 1 + width, :]
    spread -= 4.0 * middle
    return 2.0 * middle - before[row, cells, :] + speed[row, cells, :] * spread


def set_later_row(source, before, speed, row, first=-HALO, width=WIDE):
    cells = slice(LEFT + first, LEFT + first + width)
    before[row, cells, :] = later_row(source, before, speed, row, LEFT + first, width)


def own_steps(padded, end, sums, inside):
    now, before, speed = padded
    for step in range(1, STEPS):

        def pair(i, _, now=now, before=before, step=step):
            for k in range(2):
                row = HALO + step + 2 * i + k
                set_later_row(now, before, speed, row, step, COLS - 2 * step)
            return 0

        lax.fori_loop(0, (ROWS - 2 * step) // 2, pair, 0)
        now, before = before, now
    cells = slice(STEPS, COLS - STEPS)

    def last(i, total):
        for k in range(2):
            row = STEPS + 2 * i + k
            value = later_row(now, before, speed, row + HALO, LEFT + STEPS, COLS - 2 * STEPS)
            end[row, cells, :] = value
            total = total + value
            sums[row, cells, :] = total * SCALE
        return total

    zero = jnp.zeros((COLS - 2 * STEPS, MEMBERS), jnp.float32)
    inside[cells, :] = lax.fori_loop(0, INSIDE // 2, last, zero)


def first_core_kernel(_p, _e, _s, _message, *refs):
    @pl.when(lax.axis_index("core") == 0)
    def _():
        own_steps(refs[:3], *refs[4:])


def second_core_kernel(_p, _e, _s, _end, _sums, _inside, _message, *refs):
    @pl.when(lax.axis_index("core") != 0)
    def _():
        own_steps(refs[:3], *refs[3:])


def edges_kernel(_p, _e, _s, odd, even, _end, _sums, _inside, *refs):
    padded, (end, sums, inside, offsets, copies) = refs[:3], refs[3:]
    now, before, speed = padded
    for step in range(1, STEPS):
        for row in range(step, ROWS - step):
            for first in (step - STEPS, COLS - step):
                set_later_row(now, before, speed, row + HALO, first, STEPS)
        now, before = before, now
    for first in (0, COLS - STEPS):
        cells = slice(first, first + STEPS)
        total = jnp.zeros((STEPS, MEMBERS), jnp.float32)
        for row in range(STEPS, ROWS - STEPS):
            value = later_row(now, before, speed, row + HALO, LEFT + first, STEPS)
            end[row, cells, :] = value
            total = total + value
            sums[row, cells, :] = total * SCALE
        inside[cells, :] = total

    odd_x = lax.axis_index(X) % 2 == 1
    message_to_rows(padded, odd, jnp.logical_not(odd_x))
    message_to_rows(padded, even, odd_x, jnp.where(odd_x, 0, ROW_CELLS))
    now, before, speed = padded
    for first, count in ((-1, 2), (-2, 4), (-1, 4)):
        for k in range(count):
            set_later_row(now, before, speed, HALO + first + k)
            set_later_row(now, before, speed, HALO + ROWS - 1 - first - k)
        now, before = before, now
    total = jnp.zeros((COLS, MEMBERS), jnp.float32)
    for side in range(2):
        here = jnp.zeros((COLS, MEMBERS), jnp.float32)
        for k in range(STEPS):
            row = side * (ROWS - STEPS) + k
            value = later_row(now, before, speed, row + HALO, LEFT, COLS)
            end[row] = value
            here = here + value
            sums[row] = here * SCALE
        total = total + here
        if side == 0:
            offsets[0] = total * SCALE
            total = total + inside[:COLS]
            offsets[1] = total * SCALE
    for k in range(copies.shape[0]):
        copies[k] = total


def middle_kernel(row, copies, before):
    here = lax.axis_index(X)
    total = jnp.zeros((COLS, MEMBERS), jnp.float32)
    for k in range(row.shape[0]):
        before[...] = jnp.where(k == here, total, before[...])
        total = total + row[k]
    for k in range(copies.shape[0]):
        copies[k] = total


def final_kernel(rows, before, sums, offsets, end, potential_out, end_out, potential, sems):
    copies = [pltpu.make_async_copy(end, end_out, sems.at[FINAL_PIECES])]
    copies[0].start()
    here = lax.axis_index("y")
    total = before[...]
    for k in range(rows.shape[0]):
        total = total + jnp.where(k < here, rows[k], 0.0)
    total = total * SCALE
    inner = total + offsets[0]
    upper = total + offsets[1]
    piece = ROWS // FINAL_PIECES
    for part in range(FINAL_PIECES):
        for row in range(part * piece, (part + 1) * piece):
            below = total if row < STEPS else inner if row < ROWS - STEPS else upper
            potential[row] = sums[row] + below
        place = pl.ds(part * piece, piece)
        copy = pltpu.make_async_copy(potential.at[place], potential_out.at[place], sems.at[part])
        copy.start()
        copies.append(copy)
    for copy in copies:
        copy.wait()


def on_device(pressure, earlier, speed_square):
    args = [pltpu.with_memory_space_constraint(a, pltpu.HBM) for a in (pressure, earlier, speed_square)]
    outer = call(
        outer_kernel,
        in_vmem(DEEP * ROWS),
        "outer",
        args,
        [HBM] * 3,
        VMEM,
        [in_vmem(3, ROWS + 1, TILE), pltpu.SemaphoreType.DMA((3,))],
    )
    chips, ys, xs = (lax.axis_size(name) for name in ("z", "y", X))
    swap = lambda pairs: pairs + [(b, a) for a, b in pairs]
    outer = lax.ppermute(outer, LON, swap([(2 * z + 1, 2 * z + 2) for z in range(chips - 1)]))
    *padded, inner = call(
        load_kernel,
        [PADDED] * 3 + [RAW] * 3 + [in_vmem(DEEP * ROWS)],
        "load",
        [pltpu.with_memory_space_constraint(a, pltpu.VMEM) for a in (pressure, earlier, speed_square)],
        [VMEM] * 3,
        [VMEM] * 7,
    )
    padded, raw = padded[:3], padded[3:]
    same = {0: 0, 1: 1, 2: 2}
    *padded, inner, end, sums, inside = call(
        first_core_kernel,
        [PADDED] * 3 + [in_vmem(DEEP * ROWS)] + [in_vmem(ROWS, COLS)] * 2 + [in_vmem(COLS + 8)],
        "own0",
        (*padded, inner),
        [VMEM] * 4,
        [VMEM] * 7,
        aliases={**same, 3: 3},
    )
    inner = lax.all_gather(inner, "core", axis=0, tiled=True)
    *padded, end, sums, inside = call(
        second_core_kernel,
        [PADDED] * 3 + [in_vmem(ROWS, COLS)] * 2 + [in_vmem(COLS + 8)],
        "own1",
        (*padded, end, sums, inside, inner),
        [VMEM] * 7,
        [VMEM] * 6,
        aliases={k: k for k in range(6)},
        flops=10**8,
    )
    *padded, odd, even = call(
        columns_kernel,
        [PADDED] * 3 + [RAW] * 3 + [in_vmem(ROW_CELLS)] * 2,
        "columns",
        (*padded, *raw, outer, inner),
        [VMEM] * 8,
        [VMEM] * 8,
        aliases={k: k for k in range(6)},
    )
    padded = padded[:3]
    blocks = ys * xs
    odd = lax.ppermute(odd, LAT, swap([(i, i + 1) for i in range(1, blocks - 1, 2)]))
    even = lax.all_gather(even, "xl", axis=0, tiled=True)
    *_, end, sums, _, offsets, copies = call(
        edges_kernel,
        [PADDED] * 3 + [in_vmem(ROWS, COLS)] * 2 + [in_vmem(COLS + 8), in_vmem(2, COLS), in_vmem(xs, COLS)],
        "edges",
        (*padded, odd, even, end, sums, inside),
        [VMEM] * 8,
        [VMEM] * 8,
        aliases={**same, 5: 3, 6: 4, 7: 5},
    )
    row = lax.all_to_all(copies, X, 0, 0, tiled=True)
    copies, before = call(
        middle_kernel,
        [in_vmem(ys, COLS), in_vmem(COLS)],
        "middle",
        (row,),
        [VMEM],
        [VMEM] * 2,
    )
    rows = lax.all_to_all(copies, "y", 0, 0, tiled=True)
    return call(
        final_kernel,
        [WHOLE] * 2,
        "final",
        (rows, before, sums, offsets, end),
        [VMEM] * 5,
        [HBM] * 2,
        [in_vmem(ROWS, COLS), pltpu.SemaphoreType.DMA((FINAL_PIECES + 1,))],
    )


def solution(mesh):
    fine = Mesh(mesh.devices.reshape(8, 2, 2, 8, 2), ("y", *X, "z", "core"))
    spec = P(LAT, LON, None)
    return jax.shard_map(
        on_device, mesh=fine, in_specs=(spec,) * 3, out_specs=(spec,) * 2, check_vma=False
    )
```
